128 devices in a mesh: row: 8 (over z, x_hi), col: 16 (over y, x_lo, core).
Axes of the slice: x: 4 (x_hi: 2, x_lo: 2; x = x_hi * 2 + x_lo), y: 4, z: 4, core: 2. Of those that a mesh axis runs over, the one named last changes fastest.
Arguments:
- node_feats: bfloat16 [16384, 512], P(('row', 'col')), may hold values from -80 to 80
- block_mask: int32 [128, 128], replicated, may hold values from 0 to 1, as said below
- w_qkv: bfloat16 [2, 512, 1536], replicated, may hold values from -0.25 to 0.25
- w_out: bfloat16 [2, 512, 512], replicated, may hold values from -0.79296875 to 0.79296875
- w_up: bfloat16 [2, 512, 1024], replicated, may hold values from -0.25 to 0.25
- w_down: bfloat16 [2, 1024, 512], replicated, may hold values from -0.1875 to 0.1875
- ln_gain: float32 [2, 2, 512], replicated, may hold values from 0.1 to 1.9
- ln_bias: float32 [2, 2, 512], replicated, may hold values from -3 to 3
Outputs:
- nodes_out: bfloat16 [16384, 512], P(('row', 'col'))
The draws below stay inside these ranges and needn't reach their ends.
Inputs may be any that keep to these rules, and one draw needn't show every extreme that they name: `block_mask`: A symmetric 0/1 table over the 128 node blocks; every block is linked with itself.
All inputs are finite; a program needn't handle non-finite values.
Results may differ from the reference program's by a relative error of at most 0.022.
Values may be sent and summed in bfloat16 or wider, within the bound.
A program may use at most 128 MiB of HBM per device.

```python
import jax
import jax.numpy as jnp
from jax import lax

D = 512
HEADS = 8
FF = 1024
BLOCK = 128
LAYERS = 2
NB = 128
NODES = 16384
N_ROW = 8


def draw_node_feats(key, part):
    base = jnp.clip(jax.random.normal(key, (NODES, D), jnp.float32), -6.0, 6.0)
    return base.astype(jnp.bfloat16)


def draw_block_mask(key, part):
    index = jnp.arange(NB, dtype=jnp.int32)
    apart = jnp.abs(index[:, None] - index[None, :])
    apart = jnp.minimum(apart, NB - apart)
    random_bits = jax.random.randint(key, (NB, NB), 0, 16, dtype=jnp.int32)
    busy = jax.random.randint(jax.random.fold_in(key, 1), (NB,), 0, 8, dtype=jnp.int32) == 0
    far_row = NB // 2
    far_col = NB // (2 * N_ROW)
    limit = jnp.where(apart <= 1, 12, jnp.where(apart <= 3, 3, 0))
    limit = jnp.where(busy[:, None] | busy[None, :], jnp.maximum(limit, 2), limit)
    limit = jnp.where((apart == far_row) | (apart == far_col), 16, limit)
    upper = random_bits < limit
    linked = upper | upper.T | (apart == 0)
    return linked.astype(jnp.int32)


def scatter_about(rng, dims, scale, most, kind=jnp.bfloat16):
    array = scale * jax.random.normal(rng, dims, jnp.float32)
    return jnp.clip(array, min=-most, max=most).astype(kind)


def setup_inputs(seed: int = 0) -> dict:
    key_of = jax.random.split(jax.random.key(seed), 9)
    return {
        "node_feats": draw_node_feats(jax.random.fold_in(key_of[8], 71), 0),
        "block_mask": draw_block_mask(jax.random.fold_in(key_of[8], 71), 0),
        "w_qkv": scatter_about(key_of[2], (LAYERS, D, 3 * D), D ** -0.5, 0.25),
        "w_out": scatter_about(key_of[3], (LAYERS, D, D), (3.0 * D ** -0.5), 0.79296875),
        "w_up": scatter_about(key_of[4], (LAYERS, D, FF), D ** -0.5, 0.25),
        "w_down": scatter_about(key_of[5], (LAYERS, FF, D), FF ** -0.5, 0.1875),
        "ln_gain": jnp.clip(1.0 + 0.18 * jax.random.normal(key_of[6], (LAYERS, 2, D), jnp.float32), 0.1, 1.9),
        "ln_bias": scatter_about(key_of[7], (LAYERS, 2, D), 0.5, 3.0, jnp.float32),
    }


def layer_norm(values, gain, bias):
    center = values - lax.optimization_barrier(jnp.mean(values, axis=-1, keepdims=True))
    spread = lax.optimization_barrier(jnp.mean(center * center, axis=-1, keepdims=True))
    return center * lax.rsqrt(spread + 1e-05) * gain + bias

def attend(queries, keys, values, block_mask):
    head_dim = D // HEADS
    qrows = 512
    qsplit = queries.astype(jnp.float32).reshape(NODES // qrows, qrows, HEADS, head_dim)
    ksplit = keys.astype(jnp.float32).reshape(NODES, HEADS, head_dim)
    vsplit = values.astype(jnp.float32).reshape(NODES, HEADS, head_dim)
    mask_rows = block_mask.reshape(NODES // qrows, qrows // BLOCK, NB)

    def one_block(item):
        qblock, mblock = item
        scores = jnp.einsum('qhd,khd->hqk', qblock, ksplit) * (1.0 / head_dim ** 0.5)
        allowed = (jnp.repeat(jnp.repeat(mblock, BLOCK, axis=0), BLOCK, axis=1) > 0)[None]
        peak = lax.optimization_barrier(jnp.max(jnp.where(allowed, scores, -1e+30), axis=-1, keepdims=True))
        weights = jnp.where(allowed, jnp.exp(scores - peak), 0.0)
        mass = lax.optimization_barrier(jnp.sum(weights, axis=-1))
        rounded = lax.optimization_barrier(weights.astype(jnp.bfloat16)).astype(jnp.float32)
        summed = jnp.einsum('hqk,khd->qhd', rounded, vsplit)
        return (summed / mass.T[:, :, None]).reshape(qrows, D).astype(jnp.bfloat16)
    return lax.map(one_block, (qsplit, mask_rows)).reshape(NODES, D)

def reference(node_feats, block_mask, w_qkv, w_out, w_up, w_down, ln_gain, ln_bias):
    x = node_feats
    for layer in range(LAYERS):
        qkv = jnp.dot(x, w_qkv[layer], preferred_element_type=jnp.float32).astype(jnp.bfloat16)
        attn = attend(qkv[:, :D], qkv[:, D:2 * D], qkv[:, 2 * D:], block_mask)
        mixed = jnp.dot(attn, w_out[layer], preferred_element_type=jnp.float32)
        hidden = layer_norm(x.astype(jnp.float32) + mixed, ln_gain[layer, 0], ln_bias[layer, 0]).astype(jnp.bfloat16)
        up = jax.nn.gelu(jnp.dot(hidden, w_up[layer], preferred_element_type=jnp.float32)).astype(jnp.bfloat16)
        down = jnp.dot(up, w_down[layer], preferred_element_type=jnp.float32)
        x = layer_norm(hidden.astype(jnp.float32) + down, ln_gain[layer, 1], ln_bias[layer, 1]).astype(jnp.bfloat16)
    return x
```

```python
import functools
import math

import jax
import jax.numpy as jnp
from jax import lax
from jax.experimental import pallas as pl
from jax.experimental.pallas import tpu as pltpu
from jax.sharding import PartitionSpec as P

MESH = pl.DeviceIdType.MESH
D = 512
HEADS = 8
FF = 1024
BLOCK = 128
LAYERS = 2
HD = D // HEADS
LOW = -1e30
SCALE = math.log2(math.e) / math.sqrt(HD)
SHORT = 44
LONG = 128


def lists_kernel(mask_ref, out_ref):
    r, c = lax.axis_index("row"), lax.axis_index("col")
    z, t = r // 2, (r % 2) * 16 + c
    f32 = jnp.float32
    mask = mask_ref[...].astype(f32)
    iota = lambda shape, d: lax.broadcasted_iota(jnp.int32, shape, d)
    one = lambda cond: jnp.where(cond, 1.0, 0.0).astype(f32)
    dims = lambda a, b: (((a,), (b,)), ((), ()))
    dot = lambda a, b, d: lax.dot_general(a, b, d, preferred_element_type=f32)
    query_sel = one(iota((8, 128), 1) == iota((8, 128), 0) * 32 + t)
    key_sel = one(iota((128, 32), 0) == iota((128, 32), 1) + z * 32)
    by_key = dot(mask, query_sel, dims(0, 1))
    sub = dot(key_sel, by_key, dims(0, 0))
    before = dot(one(iota((32, 32), 1) < iota((32, 32), 0)), sub, dims(1, 0))
    totals = jnp.sum(sub, axis=0, keepdims=True)
    lanes = iota((32, 128), 1).astype(f32)
    keys = iota((32, 128), 0).astype(f32)
    zero = jnp.zeros((1, 128), f32)
    q_row, k_row, f_row, e_row, start = zero, zero, zero, zero, jnp.zeros((1, 1), f32)
    lane = iota((1, 128), 1)
    for q in range(4):
        rank = before[:, q : q + 1] + start
        hit = jnp.where((rank == lanes) & (sub[:, q : q + 1] > 0.5), 1.0, 0.0)
        taken = jnp.sum(hit, axis=0, keepdims=True)
        q_row += taken * float(q)
        k_row += jnp.sum(hit * keys, axis=0, keepdims=True)
        f_row += jnp.where(lane.astype(f32) == start, taken, 0.0)
        total = totals[:, q : q + 1]
        last = jnp.where(total > 0.5, start + total, 0.0)
        e_row += jnp.where(lane == q, last, 0.0)
        start = start + total
    plane_t = one(iota((32, 128), 1) % 32 == iota((32, 128), 0))
    plane_z = one(iota((128, 8), 0) // 32 == iota((128, 8), 1))
    counts = dot(dot(plane_t, mask, dims(1, 0)), plane_z, dims(1, 0))
    most = jnp.max(jnp.max(counts, axis=1, keepdims=True), axis=0, keepdims=True)
    out_ref[0:1, :] = q_row.astype(jnp.int32)
    out_ref[1:2, :] = k_row.astype(jnp.int32)
    out_ref[2:3, :] = f_row.astype(jnp.int32)
    out_ref[3:4, :] = e_row.astype(jnp.int32)
    out_ref[4:8, :] = jnp.broadcast_to(most, (4, 128)).astype(jnp.int32)


def normed(values, gain, bias):
    center = values - jnp.mean(values, axis=-1, keepdims=True)
    spread = jnp.mean(center * center, axis=-1, keepdims=True)
    return center * lax.rsqrt(spread + 1e-05) * gain + bias


def layers_kernel(
    slots, meta, x_hbm, wqkv_hbm, wout_hbm, wup_hbm, wdown_hbm, gain, bias, out_ref,
    xg, xz, kbuf, vbuf, qbd, so, sm, osend, msend, orecv, mrecv, attn_t,
    wqkv, wout, wup, wdown, wq_t, wv_t,
    in_sem, w_sem, own_sem, mate_sem, z_sem, o_sem, m_sem, send_sem,
):
    f32, bf16 = jnp.float32, jnp.bfloat16
    r, c = lax.axis_index("row"), lax.axis_index("col")
    z, y, co = r // 2, c // 4, c % 2
    x = (r % 2) * 2 + (c // 2) % 2

    def device(px, py, pz, pc):
        return (pz * 2 + px // 2, py * 4 + (px % 2) * 2 + pc)

    def place(p, q):
        dx, dy = p * (1 - co) + q * co, q * (1 - co) + p * co
        return (x + dx + 8) % 4, (y + dy + 8) % 4

    def chip_of(p, q):
        px, py = place(p, q)
        return (px // 2) * 8 + py * 2 + px % 2

    def block_of(p, q):
        return chip_of(p, q) * 2 + co

    def peer(p, q):
        px, py = place(p, q)
        return device(px, py, z, co)

    def z_peer(d):
        return device(x, y, (z + d) % 4, co)

    mate = device(x, y, z, 1 - co)
    own = block_of(0, 0)

    first = [
        pltpu.make_async_copy(x_hbm, xg.at[0, own], in_sem.at[0]),
        pltpu.make_async_copy(x_hbm, xz.at[0, z], in_sem.at[1]),
    ]
    for cp in first:
        cp.start()

    def weight_copies(l):
        return [
            pltpu.make_async_copy(src.at[l], dst.at[l], w_sem.at[i, l])
            for i, (src, dst) in enumerate(
                ((wqkv_hbm, wqkv), (wout_hbm, wout), (wup_hbm, wup), (wdown_hbm, wdown))
            )
        ]

    for l in range(LAYERS):
        for cp in weight_copies(l):
            cp.start()

    barrier = pltpu.get_barrier_semaphore()
    others = [peer(1, 0), peer(-1, 0), peer(2, 0), peer(0, 1), peer(0, -1), peer(0, 2)]
    others += [z_peer(1), z_peer(2), z_peer(3), mate]
    for other in others:
        pl.semaphore_signal(barrier, inc=1, device_id=other, device_id_type=MESH)

    qbd[...] = jnp.zeros_like(qbd)
    so[0] = jnp.zeros_like(so[0])
    for row in range(4):
        sm[0, row : row + 1, :] = jnp.full((1, 256), LOW if row % 2 == 0 else 0.0, f32)
    pl.semaphore_wait(barrier, len(others))
    for cp in first:
        cp.wait()

    def layer(l, carry):
        sends = []

        def send(src, dst, sem, to):
            cp = pltpu.make_async_remote_copy(
                src_ref=src, dst_ref=dst, send_sem=send_sem.at[l, len(sends)], recv_sem=sem,
                device_id=to, device_id_type=MESH,
            )
            cp.start()
            sends.append(cp)

        def index(p, q):
            return (p % 4) * 4 + q % 4

        def pass_on(p, q, da, db):
            block = xg.at[l, block_of(p, q)]
            send(block, block, own_sem.at[l, index(p - da, q - db)], peer(da, db))

        def to_mate(p, q):
            block = xg.at[l, block_of(p, q)]
            send(block, block, mate_sem.at[l, index(p, q)], mate)

        def arrived(block, sem):
            pltpu.make_async_remote_copy(
                src_ref=block, dst_ref=block, send_sem=send_sem.at[l, 47], recv_sem=sem,
                device_id=mate, device_id_type=MESH,
            ).wait_recv()

        def got(p, q):
            arrived(xg.at[l, block_of(p, q)], own_sem.at[l, index(p, q)])

        def got_mate(p, q):
            arrived(xg.at[l, chip_of(p, q) * 2 + 1 - co], mate_sem.at[l, index(q, p)])

        pass_on(0, 0, 0, 1)
        pass_on(0, 0, 0, -1)
        pass_on(0, 0, 1, 0)
        pass_on(0, 0, -1, 0)
        pass_on(0, 0, 2, 0)
        to_mate(0, 0)
        for d in (1, 3, 2):
            send(xg.at[l, own], xz.at[l, z], z_sem.at[l, (-d) % 4], z_peer(d))

        weights = weight_copies(l)
        weights[0].wait()
        wq_t[...] = wqkv[l, :, 0:D].T
        wv_t[...] = wqkv[l, :, 2 * D : 3 * D].T

        def project(chip):
            rows = xg[l, pl.ds(chip * 2, 2)].reshape(2 * BLOCK, D)
            keys = jnp.dot(rows, wqkv[l, :, D : 2 * D], preferred_element_type=f32).astype(bf16)
            vals = lax.dot_general(
                wv_t[...], rows, (((1,), (1,)), ((), ())), preferred_element_type=f32
            ).astype(bf16)
            for i in range(2):
                for g in range(2):
                    kbuf[g, chip * 2 + i] = keys[i * BLOCK : (i + 1) * BLOCK, g * 256 : (g + 1) * 256]
                    vbuf[g, chip * 2 + i] = vals[g * 256 : (g + 1) * 256, i * BLOCK : (i + 1) * BLOCK]

        def project_all(places):
            def step(i, carry):
                p, q = places[0]
                for n, (pn, qn) in enumerate(places[1:], 1):
                    p, q = jnp.where(i == n, pn, p), jnp.where(i == n, qn, q)
                project(chip_of(p, q))
                return carry

            lax.fori_loop(0, len(places), step, 0)

        for p in (1, 3):
            got(p, 0)
            to_mate(p, 0)
            pass_on(p, 0, 0, 1)
            pass_on(p, 0, 0, -1)
        got(0, 3)
        pass_on(0, 3, 0, 1)
        to_mate(0, 3)
        got(0, 1)
        to_mate(0, 1)
        got(2, 0)
        pass_on(2, 0, 0, 1)
        pass_on(2, 0, 0, -1)
        to_mate(2, 0)
        got_mate(0, 0)
        near = [(1, 0), (3, 0), (0, 3), (0, 1)]
        for p, q in near:
            got_mate(p, q)
        project_all([(0, 0)] + near)

        for d in range(1, 4):
            arrived(xz.at[l, (z + d) % 4], z_sem.at[l, d])
        q_t = lax.dot_general(
            wq_t[...], xz[l].reshape(4 * BLOCK, D), (((1,), (1,)), ((), ())), preferred_element_type=f32
        ).astype(bf16)
        for b in range(4):
            for h in range(HEADS):
                qbd[b, h // 2, (h % 2) * HD : (h % 2 + 1) * HD, (h % 2) * BLOCK : (h % 2 + 1) * BLOCK] = q_t[
                    h * HD : (h + 1) * HD, b * BLOCK : (b + 1) * BLOCK
                ]

        got(0, 2)
        to_mate(0, 2)
        for p in (1, 3):
            got(p, 1)
            pass_on(p, 1, 0, -1)
            to_mate(p, 1)
            got(p, 3)
            to_mate(p, 3)
        got(2, 3)
        pass_on(2, 3, 0, 1)
        to_mate(2, 3)
        got(2, 1)
        to_mate(2, 1)
        diagonal = [(2, 0), (0, 2), (1, 1), (3, 1), (1, 3), (3, 3)]
        for p, q in diagonal:
            got_mate(p, q)
        project_all(diagonal)
        far = [(1, 2), (3, 2), (2, 2)]
        for p, q in far:
            got(p, q)
            to_mate(p, q)
        far = [(1, 2), (3, 2), (2, 1), (2, 3), (2, 2)]
        for p, q in far:
            got_mate(p, q)
        project_all(far)

        for g in range(2):

            def slot(s, carry):
                qi, kj = meta[0, s], meta[1, s]
                new = jnp.full((1, 256), meta[2, s], jnp.int32) > 0
                keys = kbuf[g, kj]
                vals = vbuf[g, kj]
                for pr in range(2):
                    scores = jnp.dot(
                        keys[:, pr * 128 : (pr + 1) * 128], qbd[qi, g * 2 + pr], preferred_element_type=f32
                    )
                    old = jnp.where(new, LOW, sm[s, 2 * pr : 2 * pr + 1, :])
                    top = jnp.maximum(old, jnp.max(scores, axis=0, keepdims=True))
                    keep = jnp.exp2((old - top) * SCALE)
                    p = jnp.exp2((scores - top) * SCALE)
                    mass = sm[s, 2 * pr + 1 : 2 * pr + 2, :] * keep + jnp.sum(p, axis=0, keepdims=True)
                    sm[s + 1, 2 * pr : 2 * pr + 1, :] = top
                    sm[s + 1, 2 * pr + 1 : 2 * pr + 2, :] = mass
                    pb = p.astype(bf16)
                    for hh in range(2):
                        at = (pr * 2 + hh) * HD
                        part = jnp.dot(
                            vals[at : at + HD, :], pb[:, hh * 128 : (hh + 1) * 128], preferred_element_type=f32
                        )
                        so[s + 1, at : at + HD, :] = (
                            so[s, at : at + HD, :] * keep[:, hh * 128 : (hh + 1) * 128] + part
                        )
                return carry

            lax.fori_loop(0, slots, slot, 0)
            for d in (2, 1, 3):
                pz = (z + d) % 4
                e = meta[3, pz]
                osend[l, g, d] = so[e].astype(bf16)
                msend[l, g, d] = sm[e]
                send(osend.at[l, g, d], orecv.at[l, g, z], o_sem.at[l, g, (-d) % 4], z_peer(d))
                send(msend.at[l, g, d], mrecv.at[l, g, z], m_sem.at[l, g, (-d) % 4], z_peer(d))
            e = meta[3, z]
            orecv[l, g, z] = so[e].astype(bf16)
            mrecv[l, g, z] = sm[e]

        for cp in weights[1:]:
            cp.wait()
        for g in range(2):
            for d in range(1, 4):
                pz = (z + d) % 4
                arrived(orecv.at[l, g, pz], o_sem.at[l, g, d])
                arrived(mrecv.at[l, g, pz], m_sem.at[l, g, d])
            for pr in range(2):
                tops = [mrecv[l, g, i, 2 * pr : 2 * pr + 1, :] for i in range(4)]
                top = jnp.maximum(jnp.maximum(tops[0], tops[1]), jnp.maximum(tops[2], tops[3]))
                shares = [jnp.exp2((tops[i] - top) * SCALE) for i in range(4)]
                mass = sum(shares[i] * mrecv[l, g, i, 2 * pr + 1 : 2 * pr + 2, :] for i in range(4))
                shares = [share / mass for share in shares]
                for hh in range(2):
                    at = (pr * 2 + hh) * HD
                    half = slice(hh * 128, (hh + 1) * 128)
                    attn_t[g * 256 + at : g * 256 + at + HD, :] = sum(
                        orecv[l, g, i, at : at + HD, :].astype(f32) * shares[i][:, half] for i in range(4)
                    ).astype(bf16)

        mixed = lax.dot_general(
            attn_t[...], wout[l], (((0,), (0,)), ((), ())), preferred_element_type=f32
        )
        hidden = normed(xg[l, own].astype(f32) + mixed, gain[l, 0:1, :], bias[l, 0:1, :]).astype(bf16)
        up = jax.nn.gelu(jnp.dot(hidden, wup[l], preferred_element_type=f32)).astype(bf16)
        down = jnp.dot(up, wdown[l], preferred_element_type=f32)
        result = normed(hidden.astype(f32) + down, gain[l, 1:2, :], bias[l, 1:2, :]).astype(bf16)

        @pl.when(l == 0)
        def _():
            xg[1, own] = result
            xz[1, z] = result

        @pl.when(l == 1)
        def _():
            out_ref[...] = result

        for cp in sends:
            cp.wait_send()
        return carry

    lax.fori_loop(0, LAYERS, layer, 0)


def run_layers(slots, collective_id, meta, *arrays):
    vmem, bf16, f32 = pltpu.VMEM, jnp.bfloat16, jnp.float32
    dma = pltpu.SemaphoreType.DMA
    anywhere = pl.BlockSpec(memory_space=pl.ANY)
    whole = pl.BlockSpec(memory_space=pltpu.VMEM)
    return pl.pallas_call(
        functools.partial(layers_kernel, slots),
        out_shape=jax.ShapeDtypeStruct((BLOCK, D), bf16),
        in_specs=[pl.BlockSpec(memory_space=pltpu.SMEM)] + [anywhere] * 5 + [whole] * 2,
        out_specs=whole,
        scratch_shapes=[
            vmem((2, 32, BLOCK, D), bf16),
            vmem((2, 4, BLOCK, D), bf16),
            vmem((2, 32, BLOCK, 256), bf16),
            vmem((2, 32, 256, BLOCK), bf16),
            vmem((4, 4, 128, 256), bf16),
            vmem((slots + 1, 256, 128), f32),
            vmem((slots + 1, 4, 256), f32),
            vmem((2, 2, 4, 256, 128), bf16),
            vmem((2, 2, 4, 4, 256), f32),
            vmem((2, 2, 4, 256, 128), bf16),
            vmem((2, 2, 4, 4, 256), f32),
            vmem((D, BLOCK), bf16),
            vmem((2, D, 3 * D), bf16),
            vmem((2, D, D), bf16),
            vmem((2, D, FF), bf16),
            vmem((2, FF, D), bf16),
            vmem((D, D), bf16),
            vmem((D, D), bf16),
            dma((2,)),
            dma((4, 2)),
            dma((2, 16)),
            dma((2, 16)),
            dma((2, 4)),
            dma((2, 2, 4)),
            dma((2, 2, 4)),
            dma((2, 48)),
        ],
        compiler_params=pltpu.CompilerParams(
            collective_id=collective_id, has_side_effects=True, vmem_limit_bytes=60 * 1024 * 1024
        ),
        name=f"layers_{slots}",
    )(meta, *arrays)


def per_device(node_feats, block_mask, w_qkv, w_out, w_up, w_down, ln_gain, ln_bias):
    meta = pl.pallas_call(
        lists_kernel,
        out_shape=jax.ShapeDtypeStruct((8, 128), jnp.int32),
        in_specs=[pl.BlockSpec(memory_space=pltpu.VMEM)],
        out_specs=pl.BlockSpec(memory_space=pltpu.VMEM),
        name="lists",
    )(block_mask)
    return lax.cond(
        meta[4, 0] <= SHORT,
        functools.partial(run_layers, SHORT, 0),
        functools.partial(run_layers, LONG, 1),
        meta, node_feats, w_qkv, w_out, w_up, w_down, ln_gain, ln_bias,
    )


def solution(mesh):
    placed = (P(("row", "col"), None), P(), P(), P(), P(), P(), P(), P())
    return jax.shard_map(
        per_device, mesh=mesh, in_specs=placed, out_specs=P(("row", "col"), None), check_vma=False
    )
```

```python
import functools
import math

import jax
import jax.numpy as jnp
from jax import lax
from jax.experimental import pallas as pl
from jax.experimental.pallas import tpu as pltpu
from jax.sharding import PartitionSpec as P

MESH = pl.DeviceIdType.MESH
D = 512
HEADS = 8
FF = 1024
BLOCK = 128
LAYERS = 2
HD = D // HEADS
LOW = -1e30
SCALE = math.log2(math.e) / math.sqrt(HD)
SHORT = 44
LONG = 128
STEP = {SHORT: 22, LONG: 8}


def lists_kernel(mask_ref, out_ref):
    r, c = lax.axis_index("row"), lax.axis_index("col")
    z, t = r // 2, (r % 2) * 16 + c
    f32 = jnp.float32
    mask = mask_ref[...].astype(f32)
    iota = lambda shape, d: lax.broadcasted_iota(jnp.int32, shape, d)
    one = lambda cond: jnp.where(cond, 1.0, 0.0).astype(f32)
    dims = lambda a, b: (((a,), (b,)), ((), ()))
    dot = lambda a, b, d: lax.dot_general(a, b, d, preferred_element_type=f32)
    query_sel = one(iota((8, 128), 1) == iota((8, 128), 0) * 32 + t)
    key_sel = one(iota((128, 32), 0) == iota((128, 32), 1) + z * 32)
    by_key = dot(mask, query_sel, dims(0, 1))
    sub = dot(key_sel, by_key, dims(0, 0))
    before = dot(one(iota((32, 32), 1) < iota((32, 32), 0)), sub, dims(1, 0))
    totals = jnp.sum(sub, axis=0, keepdims=True)
    lanes = iota((32, 128), 1).astype(f32)
    keys = iota((32, 128), 0).astype(f32)
    zero = jnp.zeros((1, 128), f32)
    q_row, k_row, f_row, e_row, start = zero, zero, zero, zero, jnp.zeros((1, 1), f32)
    lane = iota((1, 128), 1)
    for q in range(4):
        rank = before[:, q : q + 1] + start
        hit = jnp.where((rank == lanes) & (sub[:, q : q + 1] > 0.5), 1.0, 0.0)
        taken = jnp.sum(hit, axis=0, keepdims=True)
        q_row += taken * float(q)
        k_row += jnp.sum(hit * keys, axis=0, keepdims=True)
        f_row += jnp.where(lane.astype(f32) == start, taken, 0.0)
        total = totals[:, q : q + 1]
        last = jnp.where(total > 0.5, start + total, 0.0)
        e_row += jnp.where(lane == q, last, 0.0)
        start = start + total
    plane_t = one(iota((32, 128), 1) % 32 == iota((32, 128), 0))
    plane_z = one(iota((128, 8), 0) // 32 == iota((128, 8), 1))
    counts = dot(dot(plane_t, mask, dims(1, 0)), plane_z, dims(1, 0))
    most = jnp.max(jnp.max(counts, axis=1, keepdims=True), axis=0, keepdims=True)
    out_ref[0:1, :] = q_row.astype(jnp.int32)
    out_ref[1:2, :] = k_row.astype(jnp.int32)
    out_ref[2:3, :] = f_row.astype(jnp.int32)
    out_ref[3:4, :] = e_row.astype(jnp.int32)
    out_ref[4:8, :] = jnp.broadcast_to(most, (4, 128)).astype(jnp.int32)


def normed(values, gain, bias):
    center = values - jnp.mean(values, axis=-1, keepdims=True)
    spread = jnp.mean(center * center, axis=-1, keepdims=True)
    return center * lax.rsqrt(spread + 1e-05) * gain + bias


def layers_kernel(
    slots, meta, x_hbm, wqkv_hbm, wout_hbm, wup_hbm, wdown_hbm, gain, bias, out_ref,
    xg, xz, kbuf, vbuf, qbd, so, sm, osend, msend, orecv, mrecv, attn_t,
    wqkv, wout, wup, wdown, wq_t, wv_t,
    in_sem, w_sem, own_sem, mate_sem, z_sem, o_sem, m_sem, send_sem,
):
    f32, bf16 = jnp.float32, jnp.bfloat16
    r, c = lax.axis_index("row"), lax.axis_index("col")
    z, y, co = r // 2, c // 4, c % 2
    x = (r % 2) * 2 + (c // 2) % 2

    def device(px, py, pz, pc):
        return (pz * 2 + px // 2, py * 4 + (px % 2) * 2 + pc)

    def place(p, q):
        dx, dy = p * (1 - co) + q * co, q * (1 - co) + p * co
        return (x + dx + 8) % 4, (y + dy + 8) % 4

    def chip_of(p, q):
        px, py = place(p, q)
        return (px // 2) * 8 + py * 2 + px % 2

    def block_of(p, q):
        return chip_of(p, q) * 2 + co

    def peer(p, q):
        px, py = place(p, q)
        return device(px, py, z, co)

    def z_peer(d):
        return device(x, y, (z + d) % 4, co)

    mate = device(x, y, z, 1 - co)
    own = block_of(0, 0)

    first = [
        pltpu.make_async_copy(x_hbm, xg.at[0, own], in_sem.at[0]),
        pltpu.make_async_copy(x_hbm, xz.at[0, z], in_sem.at[1]),
    ]
    for cp in first:
        cp.start()

    def weight_copies(l):
        return [
            pltpu.make_async_copy(src.at[l], dst.at[l], w_sem.at[i, l])
            for i, (src, dst) in enumerate(
                ((wqkv_hbm, wqkv), (wout_hbm, wout), (wup_hbm, wup), (wdown_hbm, wdown))
            )
        ]

    for l in range(LAYERS):
        for cp in weight_copies(l):
            cp.start()

    barrier = pltpu.get_barrier_semaphore()
    others = [peer(1, 0), peer(-1, 0), peer(2, 0), peer(0, 1), peer(0, -1), peer(0, 2)]
    others += [z_peer(1), z_peer(2), z_peer(3), mate]
    for other in others:
        pl.semaphore_signal(barrier, inc=1, device_id=other, device_id_type=MESH)

    qbd[...] = jnp.zeros_like(qbd)
    so[0] = jnp.zeros_like(so[0])
    for row in range(4):
        sm[0, row : row + 1, :] = jnp.full((1, 256), LOW if row % 2 == 0 else 0.0, f32)
    pl.semaphore_wait(barrier, len(others))
    for cp in first:
        cp.wait()

    def layer(l, carry):
        sends = []

        def send(src, dst, sem, to):
            cp = pltpu.make_async_remote_copy(
                src_ref=src, dst_ref=dst, send_sem=send_sem.at[l, len(sends)], recv_sem=sem,
                device_id=to, device_id_type=MESH,
            )
            cp.start()
            sends.append(cp)

        def index(p, q):
            return (p % 4) * 4 + q % 4

        def pass_on(p, q, da, db):
            block = xg.at[l, block_of(p, q)]
            send(block, block, own_sem.at[l, index(p - da, q - db)], peer(da, db))

        def to_mate(p, q):
            block = xg.at[l, block_of(p, q)]
            send(block, block, mate_sem.at[l, index(p, q)], mate)

        def arrived(block, sem):
            pltpu.make_async_remote_copy(
                src_ref=block, dst_ref=block, send_sem=send_sem.at[l, 47], recv_sem=sem,
                device_id=mate, device_id_type=MESH,
            ).wait_recv()

        def got(p, q):
            arrived(xg.at[l, block_of(p, q)], own_sem.at[l, index(p, q)])

        def got_mate(p, q):
            arrived(xg.at[l, chip_of(p, q) * 2 + 1 - co], mate_sem.at[l, index(q, p)])

        pass_on(0, 0, 0, 1)
        pass_on(0, 0, 0, -1)
        pass_on(0, 0, 1, 0)
        pass_on(0, 0, -1, 0)
        pass_on(0, 0, 2, 0)
        to_mate(0, 0)
        for d in (1, 3, 2):
            send(xg.at[l, own], xz.at[l, z], z_sem.at[l, (-d) % 4], z_peer(d))

        weights = weight_copies(l)
        weights[0].wait()
        wq_t[...] = wqkv[l, :, 0:D].T
        wv_t[...] = wqkv[l, :, 2 * D : 3 * D].T

        def project(chip):
            rows = xg[l, pl.ds(chip * 2, 2)].reshape(2 * BLOCK, D)
            keys = jnp.dot(rows, wqkv[l, :, D : 2 * D], preferred_element_type=f32).astype(bf16)
            vals = lax.dot_general(
                wv_t[...], rows, (((1,), (1,)), ((), ())), preferred_element_type=f32
            ).astype(bf16)
            for i in range(2):
                for g in range(2):
                    kbuf[g, chip * 2 + i] = keys[i * BLOCK : (i + 1) * BLOCK, g * 256 : (g + 1) * 256]
                    vbuf[g, chip * 2 + i] = vals[g * 256 : (g + 1) * 256, i * BLOCK : (i + 1) * BLOCK]

        def project_all(places):
            def step(i, carry):
                p, q = places[0]
                for n, (pn, qn) in enumerate(places[1:], 1):
                    p, q = jnp.where(i == n, pn, p), jnp.where(i == n, qn, q)
                project(chip_of(p, q))
                return carry

            lax.fori_loop(0, len(places), step, 0)

        for p in (1, 3):
            got(p, 0)
            to_mate(p, 0)
            pass_on(p, 0, 0, 1)
            pass_on(p, 0, 0, -1)
        got(0, 3)
        pass_on(0, 3, 0, 1)
        to_mate(0, 3)
        got(0, 1)
        to_mate(0, 1)
        got(2, 0)
        pass_on(2, 0, 0, 1)
        pass_on(2, 0, 0, -1)
        to_mate(2, 0)
        got_mate(0, 0)
        near = [(1, 0), (3, 0), (0, 3), (0, 1)]
        for p, q in near:
            got_mate(p, q)
        project_all([(0, 0)] + near)

        for d in range(1, 4):
            arrived(xz.at[l, (z + d) % 4], z_sem.at[l, d])
        q_t = lax.dot_general(
            wq_t[...], xz[l].reshape(4 * BLOCK, D), (((1,), (1,)), ((), ())), preferred_element_type=f32
        ).astype(bf16)
        for b in range(4):
            for h in range(HEADS):
                qbd[b, h // 2, (h % 2) * HD : (h % 2 + 1) * HD, (h % 2) * BLOCK : (h % 2 + 1) * BLOCK] = q_t[
                    h * HD : (h + 1) * HD, b * BLOCK : (b + 1) * BLOCK
                ]

        got(0, 2)
        to_mate(0, 2)
        for p in (1, 3):
            got(p, 1)
            pass_on(p, 1, 0, -1)
            to_mate(p, 1)
            got(p, 3)
            to_mate(p, 3)
        got(2, 3)
        pass_on(2, 3, 0, 1)
        to_mate(2, 3)
        got(2, 1)
        to_mate(2, 1)
        diagonal = [(2, 0), (0, 2), (1, 1), (3, 1), (1, 3), (3, 3)]
        for p, q in diagonal:
            got_mate(p, q)
        project_all(diagonal)
        far = [(1, 2), (3, 2), (2, 2)]
        for p, q in far:
            got(p, q)
            to_mate(p, q)
        far = [(1, 2), (3, 2), (2, 1), (2, 3), (2, 2)]
        for p, q in far:
            got_mate(p, q)
        project_all(far)

        for g in range(2):

            def slot(s):
                qi, kj = meta[0, s], meta[1, s]
                new = jnp.full((1, 256), meta[2, s], jnp.int32) > 0
                keys = kbuf[g, kj]
                vals = vbuf[g, kj]
                for pr in range(2):
                    scores = jnp.dot(
                        keys[:, pr * 128 : (pr + 1) * 128], qbd[qi, g * 2 + pr], preferred_element_type=f32
                    )
                    old = jnp.where(new, LOW, sm[s, 2 * pr : 2 * pr + 1, :])
                    top = jnp.maximum(old, jnp.max(scores, axis=0, keepdims=True))
                    keep = jnp.exp2((old - top) * SCALE)
                    p = jnp.exp2((scores - top) * SCALE)
                    mass = sm[s, 2 * pr + 1 : 2 * pr + 2, :] * keep + jnp.sum(p, axis=0, keepdims=True)
                    sm[s + 1, 2 * pr : 2 * pr + 1, :] = top
                    sm[s + 1, 2 * pr + 1 : 2 * pr + 2, :] = mass
                    pb = p.astype(bf16)
                    for hh in range(2):
                        at = (pr * 2 + hh) * HD
                        part = jnp.dot(
                            vals[at : at + HD, :], pb[:, hh * 128 : (hh + 1) * 128], preferred_element_type=f32
                        )
                        so[s + 1, at : at + HD, :] = (
                            so[s, at : at + HD, :] * keep[:, hh * 128 : (hh + 1) * 128] + part
                        )

            def steps(i, carry):
                for n in range(STEP[slots]):
                    slot(i * STEP[slots] + n)
                return carry

            lax.fori_loop(0, slots // STEP[slots], steps, 0)
            for d in (2, 1, 3):
                pz = (z + d) % 4
                e = meta[3, pz]
                osend[l, g, d] = so[e].astype(bf16)
                msend[l, g, d] = sm[e]
                send(osend.at[l, g, d], orecv.at[l, g, z], o_sem.at[l, g, (-d) % 4], z_peer(d))
                send(msend.at[l, g, d], mrecv.at[l, g, z], m_sem.at[l, g, (-d) % 4], z_peer(d))
            e = meta[3, z]
            orecv[l, g, z] = so[e].astype(bf16)
            mrecv[l, g, z] = sm[e]

        for cp in weights[1:]:
            cp.wait()
        for g in range(2):
            for d in range(1, 4):
                pz = (z + d) % 4
                arrived(orecv.at[l, g, pz], o_sem.at[l, g, d])
                arrived(mrecv.at[l, g, pz], m_sem.at[l, g, d])
            for pr in range(2):
                tops = [mrecv[l, g, i, 2 * pr : 2 * pr + 1, :] for i in range(4)]
                top = jnp.maximum(jnp.maximum(tops[0], tops[1]), jnp.maximum(tops[2], tops[3]))
                shares = [jnp.exp2((tops[i] - top) * SCALE) for i in range(4)]
                mass = sum(shares[i] * mrecv[l, g, i, 2 * pr + 1 : 2 * pr + 2, :] for i in range(4))
                shares = [share / mass for share in shares]
                for hh in range(2):
                    at = (pr * 2 + hh) * HD
                    half = slice(hh * 128, (hh + 1) * 128)
                    attn_t[g * 256 + at : g * 256 + at + HD, :] = sum(
                        orecv[l, g, i, at : at + HD, :].astype(f32) * shares[i][:, half] for i in range(4)
                    ).astype(bf16)

        mixed = lax.dot_general(
            attn_t[...], wout[l], (((0,), (0,)), ((), ())), preferred_element_type=f32
        )
        hidden = normed(xg[l, own].astype(f32) + mixed, gain[l, 0:1, :], bias[l, 0:1, :]).astype(bf16)
        up = jax.nn.gelu(jnp.dot(hidden, wup[l], preferred_element_type=f32)).astype(bf16)
        down = jnp.dot(up, wdown[l], preferred_element_type=f32)
        result = normed(hidden.astype(f32) + down, gain[l, 1:2, :], bias[l, 1:2, :]).astype(bf16)

        @pl.when(l == 0)
        def _():
            xg[1, own] = result
            xz[1, z] = result

        @pl.when(l == 1)
        def _():
            out_ref[...] = result

        for cp in sends:
            cp.wait_send()
        return carry

    lax.fori_loop(0, LAYERS, layer, 0)


def run_layers(slots, collective_id, meta, *arrays):
    vmem, bf16, f32 = pltpu.VMEM, jnp.bfloat16, jnp.float32
    dma = pltpu.SemaphoreType.DMA
    anywhere = pl.BlockSpec(memory_space=pl.ANY)
    whole = pl.BlockSpec(memory_space=pltpu.VMEM)
    return pl.pallas_call(
        functools.partial(layers_kernel, slots),
        out_shape=jax.ShapeDtypeStruct((BLOCK, D), bf16),
        in_specs=[pl.BlockSpec(memory_space=pltpu.SMEM)] + [anywhere] * 5 + [whole] * 2,
        out_specs=whole,
        scratch_shapes=[
            vmem((2, 32, BLOCK, D), bf16),
            vmem((2, 4, BLOCK, D), bf16),
            vmem((2, 32, BLOCK, 256), bf16),
            vmem((2, 32, 256, BLOCK), bf16),
            vmem((4, 4, 128, 256), bf16),
            vmem((slots + 1, 256, 128), f32),
            vmem((slots + 1, 4, 256), f32),
            vmem((2, 2, 4, 256, 128), bf16),
            vmem((2, 2, 4, 4, 256), f32),
            vmem((2, 2, 4, 256, 128), bf16),
            vmem((2, 2, 4, 4, 256), f32),
            vmem((D, BLOCK), bf16),
            vmem((2, D, 3 * D), bf16),
            vmem((2, D, D), bf16),
            vmem((2, D, FF), bf16),
            vmem((2, FF, D), bf16),
            vmem((D, D), bf16),
            vmem((D, D), bf16),
            dma((2,)),
            dma((4, 2)),
            dma((2, 16)),
            dma((2, 16)),
            dma((2, 4)),
            dma((2, 2, 4)),
            dma((2, 2, 4)),
            dma((2, 48)),
        ],
        compiler_params=pltpu.CompilerParams(
            collective_id=collective_id, has_side_effects=True, vmem_limit_bytes=60 * 1024 * 1024
        ),
        name=f"layers_{slots}",
    )(meta, *arrays)


def per_device(node_feats, block_mask, w_qkv, w_out, w_up, w_down, ln_gain, ln_bias):
    meta = pl.pallas_call(
        lists_kernel,
        out_shape=jax.ShapeDtypeStruct((8, 128), jnp.int32),
        in_specs=[pl.BlockSpec(memory_space=pltpu.VMEM)],
        out_specs=pl.BlockSpec(memory_space=pltpu.VMEM),
        name="lists",
    )(block_mask)
    return lax.cond(
        meta[4, 0] <= SHORT,
        functools.partial(run_layers, SHORT, 0),
        functools.partial(run_layers, LONG, 1),
        meta, node_feats, w_qkv, w_out, w_up, w_down, ln_gain, ln_bias,
    )


def solution(mesh):
    placed = (P(("row", "col"), None), P(), P(), P(), P(), P(), P(), P())
    return jax.shard_map(
        per_device, mesh=mesh, in_specs=placed, out_specs=P(("row", "col"), None), check_vma=False
    )
```

```python
import functools
import math

import jax
import jax.numpy as jnp
from jax import lax
from jax.experimental import pallas as pl
from jax.experimental.pallas import tpu as pltpu
from jax.sharding import PartitionSpec as P

MESH = pl.DeviceIdType.MESH
D = 512
HEADS = 8
FF = 1024
BLOCK = 128
LAYERS = 2
HD = D // HEADS
LOW = -1e30
SCALE = math.log2(math.e) / math.sqrt(HD)
H = 2
NSEND = 104
SHORT = (36, 36)
LONG = (112, 144)
STEP = {36: 36, 112: 16, 144: 16}
SLOTS = 256


def in_line(a, b):
    same_x = (a >> 3) * 2 + (a & 1) == (b >> 3) * 2 + (b & 1)
    return jnp.where(same_x | (((a >> 1) & 3) == ((b >> 1) & 3)), 1.0, 0.0)


def lists_kernel(mask_ref, out_ref, fits_ref):
    r, c = lax.axis_index("row"), lax.axis_index("col")
    z, chip = r // 2, (r % 2) * 8 + c // 2
    f32 = jnp.float32
    mask = mask_ref[...].astype(f32)
    iota = lambda shape, d: lax.broadcasted_iota(jnp.int32, shape, d)
    one = lambda cond: jnp.where(cond, 1.0, 0.0).astype(f32)
    dims = lambda a, b: (((a,), (b,)), ((), ()))
    dot = lambda a, b, d: lax.dot_general(a, b, d, preferred_element_type=f32)
    plane_chip = one(((iota((16, 128), 1) & 31) >> 1) == iota((16, 128), 0))
    plane_z = one((iota((128, 8), 0) >> 5) == iota((128, 8), 1))
    close = in_line(iota((16, 128), 0), (iota((16, 128), 1) & 31) >> 1)
    linked = dot(plane_chip, mask, dims(1, 0))
    near_most = jnp.max(dot(linked * close, plane_z, dims(1, 0)))
    far_most = jnp.max(dot(linked * (1.0 - close), plane_z, dims(1, 0)))
    fits = (near_most <= SHORT[0]) & (far_most <= SHORT[1])
    fits_ref[0, 0] = fits.astype(jnp.int32)

    b = iota((8, 128), 0)
    query_sel = one(iota((8, 128), 1) == (b >> 1) * 32 + chip * 2 + (b & 1))
    key_sel = one(iota((128, 32), 0) == iota((128, 32), 1) + z * 32)
    sub = dot(key_sel, dot(mask, query_sel, dims(0, 1)), dims(0, 0))
    near = in_line(iota((32, 8), 0) >> 1, chip)
    earlier = one(iota((32, 32), 1) < iota((32, 32), 0))
    lanes = iota((32, SLOTS), 1).astype(f32)
    keys = iota((32, SLOTS), 0).astype(f32)
    lane = iota((1, SLOTS), 1).astype(f32)
    zero = jnp.zeros((1, SLOTS), f32)
    rows, last = [], [jnp.zeros((1, 1), f32)] * 8
    for group in (sub * near, sub * (1.0 - near)):
        q_row = k_row = n_row = p_row = e_row = zero
        before = dot(earlier, group, dims(1, 0))
        totals = jnp.sum(group, axis=0, keepdims=True)
        start = jnp.zeros((1, 1), f32)
        for q in range(8):
            rank = before[:, q : q + 1] + start
            hit = jnp.where((rank == lanes) & (group[:, q : q + 1] > 0.5), 1.0, 0.0)
            taken = jnp.sum(hit, axis=0, keepdims=True)
            q_row += taken * float(q)
            k_row += jnp.sum(hit * keys, axis=0, keepdims=True)
            fresh = jnp.where(lane == start, taken, 0.0)
            n_row += fresh
            p_row += fresh * last[q]
            total = totals[:, q : q + 1]
            last[q] = jnp.where(total > 0.5, start + total, 0.0)
            e_row += jnp.where(lane == float(q), last[q], 0.0)
            start = start + total
        rows += [q_row, k_row, n_row, p_row, e_row]
    for n, row in enumerate(rows):
        out_ref[n : n + 1, :] = row.astype(jnp.int32)
    out_ref[10:16, :] = jnp.zeros((6, SLOTS), jnp.int32)


def normed(values, gain, bias):
    center = values - jnp.mean(values, axis=-1, keepdims=True)
    spread = jnp.mean(center * center, axis=-1, keepdims=True)
    return center * lax.rsqrt(spread + 1e-05) * gain + bias


def layers_kernel(
    counts, meta, x_hbm, wqkv_hbm, wout_hbm, wup_hbm, wdown_hbm, gain, bias, out_ref,
    xg, xz, kbuf, vbuf, qbd, so, sm, so_far, sm_far, osend, msend, orecv, mrecv, attn_t,
    wqkv, wout, wup, wdown, wq_t, wv_t,
    in_sem, w_sem, own_sem, mate_sem, z_sem, zm_sem, o_sem, m_sem, send_sem,
):
    f32, bf16 = jnp.float32, jnp.bfloat16
    r, c = lax.axis_index("row"), lax.axis_index("col")
    z, y, co = r // 2, c // 4, c % 2
    x = (r % 2) * 2 + (c // 2) % 2
    rows_of = BLOCK // H

    def device(px, py, pz, pc):
        return (pz * 2 + px // 2, py * 4 + (px % 2) * 2 + pc)

    def place(p, q):
        dx, dy = p * (1 - co) + q * co, q * (1 - co) + p * co
        return (x + dx + 8) % 4, (y + dy + 8) % 4

    def chip_of(p, q):
        px, py = place(p, q)
        return (px // 2) * 8 + py * 2 + px % 2

    def block_of(p, q):
        return chip_of(p, q) * 2 + co

    def peer(p, q):
        px, py = place(p, q)
        return device(px, py, z, co)

    def z_peer(d, core):
        return device(x, y, (z + d) % 4, core)

    mate = device(x, y, z, 1 - co)
    own = block_of(0, 0)

    first = [
        pltpu.make_async_copy(x_hbm, xg.at[0, own], in_sem.at[0]),
    ]
    for cp in first:
        cp.start()

    def weight_copies(l):
        return [
            pltpu.make_async_copy(src.at[l], dst.at[l], w_sem.at[i, l])
            for i, (src, dst) in enumerate(
                ((wqkv_hbm, wqkv), (wout_hbm, wout), (wup_hbm, wup), (wdown_hbm, wdown))
            )
        ]

    for l in range(LAYERS):
        for cp in weight_copies(l):
            cp.start()

    barrier = pltpu.get_barrier_semaphore()
    others = [peer(1, 0), peer(-1, 0), peer(2, 0), peer(0, 1), peer(0, -1), peer(0, 2)]
    others += [z_peer(d, core) for d in (1, 2, 3) for core in (0, 1)] + [mate]
    for other in others:
        pl.semaphore_signal(barrier, inc=1, device_id=other, device_id_type=MESH)

    qbd[...] = jnp.zeros_like(qbd)
    for sums, marks in ((so, sm), (so_far, sm_far)):
        for g in range(2):
            sums[g, 0] = jnp.zeros((128, 128), f32)
            marks[0, 2 * g : 2 * g + 1, :] = jnp.full((1, 256), LOW, f32)
            marks[0, 2 * g + 1 : 2 * g + 2, :] = jnp.zeros((1, 256), f32)
    pl.semaphore_wait(barrier, len(others))
    for cp in first:
        cp.wait()

    def layer(l, carry):
        sends = []

        def send(src, dst, sem, to):
            cp = pltpu.make_async_remote_copy(
                src_ref=src, dst_ref=dst, send_sem=send_sem.at[l, len(sends)], recv_sem=sem,
                device_id=to, device_id_type=MESH,
            )
            cp.start()
            sends.append(cp)

        def index(p, q):
            return (p % 4) * 4 + q % 4

        def piece(block, h):
            return xg.at[l, block, pl.ds(h * rows_of, rows_of)]

        def pass_on(p, q, da, db, h):
            block = piece(block_of(p, q), h)
            send(block, block, own_sem.at[l, index(p - da, q - db) * H + h], peer(da, db))

        def to_mate(p, q, h):
            block = piece(block_of(p, q), h)
            send(block, block, mate_sem.at[l, index(p, q) * H + h], mate)

        def arrived(block, sem):
            pltpu.make_async_remote_copy(
                src_ref=block, dst_ref=block, send_sem=send_sem.at[l, NSEND - 1], recv_sem=sem,
                device_id=mate, device_id_type=MESH,
            ).wait_recv()

        def got(p, q, h):
            arrived(piece(block_of(p, q), h), own_sem.at[l, index(p, q) * H + h])

        def got_mate(p, q):
            for h in range(H):
                arrived(piece(chip_of(p, q) * 2 + 1 - co, h), mate_sem.at[l, index(q, p) * H + h])

        for h in range(H):
            pass_on(0, 0, 1, 0, h)
            pass_on(0, 0, -1, 0, h)
            pass_on(0, 0, 0, 1, h)
            pass_on(0, 0, 0, -1, h)
        for h in range(H):
            pass_on(0, 0, 2, 0, h)
            pass_on(0, 0, 0, 2, h)
        for h in range(H):
            to_mate(0, 0, h)
        for d in (1, 3, 2):
            send(xg.at[l, own], xz.at[l, z * 2 + co], z_sem.at[l, (-d) % 4], z_peer(d, co))

        weights = weight_copies(l)
        weights[0].wait()
        wq_t[...] = wqkv[l, :, pl.ds(pl.multiple_of(co * 256, 256), 256)].T
        wv_t[...] = wqkv[l, :, pl.ds(pl.multiple_of(2 * D + co * 256, 256), 256)].T

        def transposed_product(weight, rows):
            return lax.dot_general(weight, rows, (((1,), (1,)), ((), ())), preferred_element_type=f32).astype(bf16)

        def project(chip):
            rows = xg[l, pl.ds(chip * 2, 2)].reshape(2 * BLOCK, D)
            keys = jnp.dot(
                rows, wqkv[l, :, pl.ds(pl.multiple_of(D + co * 256, 256), 256)], preferred_element_type=f32
            ).astype(bf16)
            vals = transposed_product(wv_t[...], rows)
            for i in range(2):
                for g in range(2):
                    kbuf[g, chip * 2 + i] = keys[i * BLOCK : (i + 1) * BLOCK, g * 128 : (g + 1) * 128]
                    vbuf[g, chip * 2 + i] = vals[g * 128 : (g + 1) * 128, i * BLOCK : (i + 1) * BLOCK]

        def project_all(places):
            for p, q in places:
                project(chip_of(p, q))

        def queries(pz, rows):
            q_t = transposed_product(wq_t[...], rows.reshape(2 * BLOCK, D))
            for core in range(2):
                for h in range(4):
                    hh = h % 2
                    qbd[pz * 2 + core, h // 2, hh * HD : (hh + 1) * HD, hh * BLOCK : (hh + 1) * BLOCK] = q_t[
                        h * HD : (h + 1) * HD, core * BLOCK : (core + 1) * BLOCK
                    ]

        for h in range(H):
            for p in (1, 3):
                got(p, 0, h)
                pass_on(p, 0, 0, 1, h)
                pass_on(p, 0, 0, -1, h)
                to_mate(p, 0, h)
        for h in range(H):
            got(2, 0, h)
            pass_on(2, 0, 0, 1, h)
            pass_on(2, 0, 0, -1, h)
            pass_on(2, 0, 0, 2, h)
            to_mate(2, 0, h)
        for h in range(H):
            for q in (1, 3):
                got(0, q, h)
                to_mate(0, q, h)
        got_mate(0, 0)
        near = [(1, 0), (3, 0), (0, 3), (0, 1)]
        for p, q in near:
            got_mate(p, q)
        project_all([(0, 0)] + near)

        for d in range(1, 4):
            block = xz.at[l, ((z + d) % 4) * 2 + co]
            arrived(block, z_sem.at[l, d])
            send(block, block, zm_sem.at[l, d], mate)
        queries(z, xg[l, pl.ds(chip_of(0, 0) * 2, 2)])
        for h in range(H):
            for p in (1, 3):
                got(p, 1, h)
                pass_on(p, 1, 0, -1, h)
                to_mate(p, 1, h)
        for h in range(H):
            got(0, 2, h)
            to_mate(0, 2, h)
        for d in range(1, 4):
            pz = (z + d) % 4
            arrived(xz.at[l, pz * 2 + 1 - co], zm_sem.at[l, d])
            queries(pz, xz[l, pl.ds(pz * 2, 2)])
        middle = [(2, 0), (0, 2)]
        for p, q in middle:
            got_mate(p, q)
        project_all(middle)

        def attend(g, far):
            sums, marks = (so_far, sm_far) if far else (so, sm)
            row, count = (5, counts[1]) if far else (0, counts[0])

            def slot(s, top_before, mass_before):
                vals = vbuf[g, meta[row + 1, s]]
                scores = jnp.dot(
                    kbuf[g, meta[row + 1, s]], qbd[meta[row, s], g], preferred_element_type=f32
                )
                new = jnp.full((1, 256), meta[row + 2, s], jnp.int32) > 0
                if far:
                    start = meta[row + 3, s]
                    top_before = jnp.where(new, sm[start, 2 * g : 2 * g + 1, :], top_before)
                    mass_before = jnp.where(new, sm[start, 2 * g + 1 : 2 * g + 2, :], mass_before)
                else:
                    top_before = jnp.where(new, LOW, top_before)
                top = jnp.maximum(top_before, jnp.max(scores, axis=0, keepdims=True))
                keep = jnp.exp2((top_before - top) * SCALE)
                p = jnp.exp2((scores - top) * SCALE)
                mass = mass_before * keep + jnp.sum(p, axis=0, keepdims=True)
                marks[s + 1, 2 * g : 2 * g + 1, :] = top
                marks[s + 1, 2 * g + 1 : 2 * g + 2, :] = mass
                pb = p.astype(bf16)
                for hh in range(2):
                    at, half = slice(hh * HD, (hh + 1) * HD), slice(hh * 128, (hh + 1) * 128)
                    part = jnp.dot(vals[at, :], pb[:, half], preferred_element_type=f32)
                    before = sums[g, s, at, :]
                    if far:
                        before = jnp.where(new[:, :128], so[g, start, at, :], before)
                    sums[g, s + 1, at, :] = before * keep[:, half] + part
                return top, mass

            def steps(i, carry):
                for n in range(STEP[count]):
                    carry = slot(i * STEP[count] + n, *carry)
                return carry

            init = (jnp.full((1, 256), LOW, f32), jnp.zeros((1, 256), f32))
            lax.fori_loop(0, count // STEP[count], steps, init)

        def state(g, b):
            near, far = meta[4, b], meta[9, b]
            take = jnp.full((1, 128), far, jnp.int32) > 0
            sums = jnp.where(take, so_far[g, far], so[g, near])
            take = jnp.full((1, 256), far, jnp.int32) > 0
            marks = jnp.where(take, sm_far[far, 2 * g : 2 * g + 2, :], sm[near, 2 * g : 2 * g + 2, :])
            return sums.astype(bf16), marks

        for g in range(2):
            attend(g, False)

        for p, q in ((1, 3), (3, 3), (2, 1), (2, 3), (1, 2), (3, 2), (2, 2)):
            for h in range(H):
                got(p, q, h)
                to_mate(p, q, h)
        far = [(1, 1), (3, 1), (1, 3), (3, 3), (1, 2), (3, 2), (2, 1), (2, 3), (2, 2)]
        for p, q in far[:4]:
            got_mate(p, q)
        project_all(far[:4])
        for p, q in far[4:]:
            got_mate(p, q)
        project_all(far[4:])

        for g in range(2):
            attend(g, True)
            for n, (d, core) in enumerate([(d, core) for d in (2, 1, 3) for core in (0, 1)] + [(0, 1 - co)]):
                osend[l, g, n], msend[l, g, n] = state(g, ((z + d) % 4) * 2 + core)
                to, at = z_peer(d, core), z * 2 + co
                sem = ((-d) % 4) * 2 + co
                send(osend.at[l, g, n], orecv.at[l, g, at], o_sem.at[l, g, sem], to)
                send(msend.at[l, g, n], mrecv.at[l, g, at], m_sem.at[l, g, sem], to)
            orecv[l, g, z * 2 + co], mrecv[l, g, z * 2 + co] = state(g, z * 2 + co)

        for cp in weights[1:]:
            cp.wait()
        for g in range(2):
            for d, core in [(0, 1 - co)] + [(d, core) for d in (1, 3, 2) for core in (0, 1)]:
                at = ((z + d) % 4) * 2 + core
                arrived(orecv.at[l, g, at], o_sem.at[l, g, d * 2 + core])
                arrived(mrecv.at[l, g, at], m_sem.at[l, g, d * 2 + core])
            for core in range(2):
                tops = [mrecv[l, g, i * 2 + core, 0:1, :] for i in range(4)]
                top = jnp.maximum(jnp.maximum(tops[0], tops[1]), jnp.maximum(tops[2], tops[3]))
                shares = [jnp.exp2((tops[i] - top) * SCALE) for i in range(4)]
                mass = sum(shares[i] * mrecv[l, g, i * 2 + core, 1:2, :] for i in range(4))
                shares = [share / mass for share in shares]
                for hh in range(2):
                    at, half = slice(hh * HD, (hh + 1) * HD), slice(hh * 128, (hh + 1) * 128)
                    to = core * 256 + g * 128 + hh * HD
                    attn_t[to : to + HD, :] = sum(
                        orecv[l, g, i * 2 + core, at, :].astype(f32) * shares[i][:, half] for i in range(4)
                    ).astype(bf16)

        mixed = lax.dot_general(
            attn_t[...], wout[l], (((0,), (0,)), ((), ())), preferred_element_type=f32
        )
        hidden = normed(xg[l, own].astype(f32) + mixed, gain[l, 0:1, :], bias[l, 0:1, :]).astype(bf16)
        up = jax.nn.gelu(jnp.dot(hidden, wup[l], preferred_element_type=f32)).astype(bf16)
        down = jnp.dot(up, wdown[l], preferred_element_type=f32)
        result = normed(hidden.astype(f32) + down, gain[l, 1:2, :], bias[l, 1:2, :]).astype(bf16)

        @pl.when(l == 0)
        def _():
            xg[1, own] = result

        @pl.when(l == 1)
        def _():
            out_ref[...] = result

        assert len(sends) < NSEND
        for cp in sends:
            cp.wait_send()
        return carry

    lax.fori_loop(0, LAYERS, layer, 0)


def run_layers(counts, collective_id, meta, *arrays):
    vmem, bf16, f32 = pltpu.VMEM, jnp.bfloat16, jnp.float32
    dma = pltpu.SemaphoreType.DMA
    anywhere = pl.BlockSpec(memory_space=pl.ANY)
    whole = pl.BlockSpec(memory_space=pltpu.VMEM)
    near, far = counts[0] + 1, counts[1] + 1
    return pl.pallas_call(
        functools.partial(layers_kernel, counts),
        out_shape=jax.ShapeDtypeStruct((BLOCK, D), bf16),
        in_specs=[pl.BlockSpec(memory_space=pltpu.SMEM)] + [anywhere] * 5 + [whole] * 2,
        out_specs=whole,
        scratch_shapes=[
            vmem((2, 32, BLOCK, D), bf16),
            vmem((2, 8, BLOCK, D), bf16),
            vmem((2, 32, BLOCK, 128), bf16),
            vmem((2, 32, 128, BLOCK), bf16),
            vmem((8, 2, 128, 256), bf16),
            vmem((2, near, 128, 128), f32),
            vmem((near, 4, 256), f32),
            vmem((2, far, 128, 128), f32),
            vmem((far, 4, 256), f32),
            vmem((2, 2, 7, 128, 128), bf16),
            vmem((2, 2, 7, 2, 256), f32),
            vmem((2, 2, 8, 128, 128), bf16),
            vmem((2, 2, 8, 2, 256), f32),
            vmem((D, BLOCK), bf16),
            vmem((2, D, 3 * D), bf16),
            vmem((2, D, D), bf16),
            vmem((2, D, FF), bf16),
            vmem((2, FF, D), bf16),
            vmem((256, D), bf16),
            vmem((256, D), bf16),
            dma((1,)),
            dma((4, 2)),
            dma((2, 16 * H)),
            dma((2, 16 * H)),
            dma((2, 4)),
            dma((2, 4)),
            dma((2, 2, 8)),
            dma((2, 2, 8)),
            dma((2, NSEND)),
        ],
        compiler_params=pltpu.CompilerParams(
            collective_id=collective_id, has_side_effects=True, vmem_limit_bytes=67043328
        ),
        name=f"layers_{near}",
    )(meta, *arrays)


def per_device(node_feats, block_mask, w_qkv, w_out, w_up, w_down, ln_gain, ln_bias):
    meta, fits = pl.pallas_call(
        lists_kernel,
        out_shape=(jax.ShapeDtypeStruct((16, SLOTS), jnp.int32), jax.ShapeDtypeStruct((1, 1), jnp.int32)),
        in_specs=[pl.BlockSpec(memory_space=pltpu.VMEM)],
        out_specs=(pl.BlockSpec(memory_space=pltpu.VMEM), pl.BlockSpec(memory_space=pltpu.SMEM)),
        name="lists",
    )(block_mask)
    return lax.cond(
        fits[0, 0] > 0,
        functools.partial(run_layers, SHORT, 0),
        functools.partial(run_layers, LONG, 1),
        meta, node_feats, w_qkv, w_out, w_up, w_down, ln_gain, ln_bias,
    )


def solution(mesh):
    placed = (P(("row", "col"), None), P(), P(), P(), P(), P(), P(), P())
    return jax.shard_map(
        per_device, mesh=mesh, in_specs=placed, out_specs=P(("row", "col"), None), check_vma=False
    )
```

```python
import functools
import math

import jax
import jax.numpy as jnp
from jax import lax
from jax.experimental import pallas as pl
from jax.experimental.pallas import tpu as pltpu
from jax.sharding import PartitionSpec as P

MESH = pl.DeviceIdType.MESH
D = 512
HEADS = 8
FF = 1024
BLOCK = 128
LAYERS = 2
HD = D // HEADS
LOW = -1e30
SCALE = math.log2(math.e) / math.sqrt(HD)
H = 1
NSEND = 104
SHORT = (36, 36)
LONG = (112, 144)
STEP = {36: 36, 112: 16, 144: 16}
SLOTS = 256


def in_line(a, b):
    same_x = (a >> 3) * 2 + (a & 1) == (b >> 3) * 2 + (b & 1)
    return jnp.where(same_x | (((a >> 1) & 3) == ((b >> 1) & 3)), 1.0, 0.0)


def lists_kernel(mask_ref, out_ref, fits_ref):
    r, c = lax.axis_index("row"), lax.axis_index("col")
    z, chip = r // 2, (r % 2) * 8 + c // 2
    f32 = jnp.float32
    mask = mask_ref[...].astype(f32)
    iota = lambda shape, d: lax.broadcasted_iota(jnp.int32, shape, d)
    one = lambda cond: jnp.where(cond, 1.0, 0.0).astype(f32)
    dims = lambda a, b: (((a,), (b,)), ((), ()))
    dot = lambda a, b, d: lax.dot_general(a, b, d, preferred_element_type=f32)
    plane_chip = one(((iota((16, 128), 1) & 31) >> 1) == iota((16, 128), 0))
    plane_z = one((iota((128, 8), 0) >> 5) == iota((128, 8), 1))
    close = in_line(iota((16, 128), 0), (iota((16, 128), 1) & 31) >> 1)
    linked = dot(plane_chip, mask, dims(1, 0))
    near_most = jnp.max(dot(linked * close, plane_z, dims(1, 0)))
    far_most = jnp.max(dot(linked * (1.0 - close), plane_z, dims(1, 0)))
    fits = (near_most <= SHORT[0]) & (far_most <= SHORT[1])
    fits_ref[0, 0] = fits.astype(jnp.int32)

    b = iota((8, 128), 0)
    query_sel = one(iota((8, 128), 1) == (b >> 1) * 32 + chip * 2 + (b & 1))
    key_sel = one(iota((128, 32), 0) == iota((128, 32), 1) + z * 32)
    sub = dot(key_sel, dot(mask, query_sel, dims(0, 1)), dims(0, 0))
    near = in_line(iota((32, 8), 0) >> 1, chip)
    earlier = one(iota((32, 32), 1) < iota((32, 32), 0))
    lanes = iota((32, SLOTS), 1).astype(f32)
    keys = iota((32, SLOTS), 0).astype(f32)
    lane = iota((1, SLOTS), 1).astype(f32)
    zero = jnp.zeros((1, SLOTS), f32)
    over_before = one(iota((8, 8), 0) < iota((8, 8), 1))
    spread = one(iota((8, SLOTS), 0) == iota((8, SLOTS), 1))
    rows, last = [], jnp.zeros((8, 8), f32)
    for group in (sub * near, sub * (1.0 - near)):
        q_row = k_row = n_row = p_row = zero
        totals = jnp.broadcast_to(jnp.sum(group, axis=0, keepdims=True), (8, 8))
        starts = dot(totals, over_before, dims(1, 0))
        ranks = dot(earlier, group, dims(1, 0)) + starts[0:1, :]
        for q in range(8):
            hit = jnp.where((ranks[:, q : q + 1] == lanes) & (group[:, q : q + 1] > 0.5), 1.0, 0.0)
            taken = jnp.sum(hit, axis=0, keepdims=True)
            q_row += taken * float(q)
            k_row += jnp.sum(hit * keys, axis=0, keepdims=True)
            fresh = jnp.where(lane == starts[0:1, q : q + 1], taken, 0.0)
            n_row += fresh
            p_row += fresh * last[0:1, q : q + 1]
        last = jnp.where(totals > 0.5, starts + totals, 0.0)
        rows += [q_row, k_row, n_row, p_row, dot(last, spread, dims(1, 0))[0:1, :]]
    for n, row in enumerate(rows):
        out_ref[n : n + 1, :] = row.astype(jnp.int32)
    out_ref[10:16, :] = jnp.zeros((6, SLOTS), jnp.int32)


def normed(values, gain, bias):
    center = values - jnp.mean(values, axis=-1, keepdims=True)
    spread = jnp.mean(center * center, axis=-1, keepdims=True)
    return center * lax.rsqrt(spread + 1e-05) * gain + bias


def layers_kernel(
    counts, meta, x_hbm, wqkv_hbm, wout_hbm, wup_hbm, wdown_hbm, gain, bias, out_ref,
    xg, xz, kbuf, vbuf, qbd, so, sm, so_far, sm_far, osend, msend, orecv, mrecv, attn_t,
    wqkv, wout, wup, wdown, wq_t, wv_t,
    in_sem, w_sem, own_sem, mate_sem, z_sem, zm_sem, o_sem, m_sem, send_sem,
):
    f32, bf16 = jnp.float32, jnp.bfloat16
    r, c = lax.axis_index("row"), lax.axis_index("col")
    z, y, co = r // 2, c // 4, c % 2
    x = (r % 2) * 2 + (c // 2) % 2
    rows_of = BLOCK // H

    def device(px, py, pz, pc):
        return (pz * 2 + px // 2, py * 4 + (px % 2) * 2 + pc)

    def place(p, q):
        dx, dy = p * (1 - co) + q * co, q * (1 - co) + p * co
        return (x + dx + 8) % 4, (y + dy + 8) % 4

    def chip_of(p, q):
        px, py = place(p, q)
        return (px // 2) * 8 + py * 2 + px % 2

    def block_of(p, q):
        return chip_of(p, q) * 2 + co

    def peer(p, q):
        px, py = place(p, q)
        return device(px, py, z, co)

    def z_peer(d, core):
        return device(x, y, (z + d) % 4, core)

    mate = device(x, y, z, 1 - co)
    own = block_of(0, 0)

    first = [
        pltpu.make_async_copy(x_hbm, xg.at[0, own], in_sem.at[0]),
    ]
    for cp in first:
        cp.start()

    def weight_copies(l):
        return [
            pltpu.make_async_copy(src.at[l], dst.at[l], w_sem.at[i, l])
            for i, (src, dst) in enumerate(
                ((wqkv_hbm, wqkv), (wout_hbm, wout), (wup_hbm, wup), (wdown_hbm, wdown))
            )
        ]

    for l in range(LAYERS):
        for cp in weight_copies(l):
            cp.start()

    barrier = pltpu.get_barrier_semaphore()
    others = [peer(1, 0), peer(-1, 0), peer(2, 0), peer(0, 1), peer(0, -1), peer(0, 2)]
    others += [z_peer(d, core) for d in (1, 2, 3) for core in (0, 1)] + [mate]
    for other in others:
        pl.semaphore_signal(barrier, inc=1, device_id=other, device_id_type=MESH)

    qbd[...] = jnp.zeros_like(qbd)
    for sums, marks in ((so, sm), (so_far, sm_far)):
        for g in range(2):
            sums[g, 0] = jnp.zeros((128, 128), f32)
            marks[0, 2 * g : 2 * g + 1, :] = jnp.full((1, 256), LOW, f32)
            marks[0, 2 * g + 1 : 2 * g + 2, :] = jnp.zeros((1, 256), f32)
    pl.semaphore_wait(barrier, len(others))
    for cp in first:
        cp.wait()

    def layer(l, carry):
        sends = []

        def send(src, dst, sem, to):
            cp = pltpu.make_async_remote_copy(
                src_ref=src, dst_ref=dst, send_sem=send_sem.at[l, len(sends)], recv_sem=sem,
                device_id=to, device_id_type=MESH,
            )
            cp.start()
            sends.append(cp)

        def index(p, q):
            return (p % 4) * 4 + q % 4

        def piece(block, h):
            return xg.at[l, block, pl.ds(h * rows_of, rows_of)]

        def pass_on(p, q, da, db, h):
            block = piece(block_of(p, q), h)
            send(block, block, own_sem.at[l, index(p - da, q - db) * H + h], peer(da, db))

        def to_mate(p, q, h):
            block = piece(block_of(p, q), h)
            send(block, block, mate_sem.at[l, index(p, q) * H + h], mate)

        def arrived(block, sem):
            pltpu.make_async_remote_copy(
                src_ref=block, dst_ref=block, send_sem=send_sem.at[l, NSEND - 1], recv_sem=sem,
                device_id=mate, device_id_type=MESH,
            ).wait_recv()

        def got(p, q, h):
            arrived(piece(block_of(p, q), h), own_sem.at[l, index(p, q) * H + h])

        def got_mate(p, q):
            for h in range(H):
                arrived(piece(chip_of(p, q) * 2 + 1 - co, h), mate_sem.at[l, index(q, p) * H + h])

        for h in range(H):
            pass_on(0, 0, 1, 0, h)
            pass_on(0, 0, -1, 0, h)
            pass_on(0, 0, 0, 1, h)
            pass_on(0, 0, 0, -1, h)
        for h in range(H):
            pass_on(0, 0, 2, 0, h)
            pass_on(0, 0, 0, 2, h)
        for h in range(H):
            to_mate(0, 0, h)
        for d in (1, 3, 2):
            send(xg.at[l, own], xz.at[l, z * 2 + co], z_sem.at[l, (-d) % 4], z_peer(d, co))

        weights = weight_copies(l)
        weights[0].wait()
        wq_t[...] = wqkv[l, :, pl.ds(pl.multiple_of(co * 256, 256), 256)].T
        wv_t[...] = wqkv[l, :, pl.ds(pl.multiple_of(2 * D + co * 256, 256), 256)].T

        def transposed_product(weight, rows):
            return lax.dot_general(weight, rows, (((1,), (1,)), ((), ())), preferred_element_type=f32).astype(bf16)

        def project(chip):
            rows = xg[l, pl.ds(chip * 2, 2)].reshape(2 * BLOCK, D)
            keys = jnp.dot(
                rows, wqkv[l, :, pl.ds(pl.multiple_of(D + co * 256, 256), 256)], preferred_element_type=f32
            ).astype(bf16)
            vals = transposed_product(wv_t[...], rows)
            for i in range(2):
                for g in range(2):
                    kbuf[g, chip * 2 + i] = keys[i * BLOCK : (i + 1) * BLOCK, g * 128 : (g + 1) * 128]
                    vbuf[g, chip * 2 + i] = vals[g * 128 : (g + 1) * 128, i * BLOCK : (i + 1) * BLOCK]

        def project_all(places):
            for p, q in places:
                project(chip_of(p, q))

        def queries(pz, rows):
            q_t = transposed_product(wq_t[...], rows.reshape(2 * BLOCK, D))
            for core in range(2):
                for h in range(4):
                    hh = h % 2
                    qbd[pz * 2 + core, h // 2, hh * HD : (hh + 1) * HD, hh * BLOCK : (hh + 1) * BLOCK] = q_t[
                        h * HD : (h + 1) * HD, core * BLOCK : (core + 1) * BLOCK
                    ]

        for h in range(H):
            for p in (1, 3):
                got(p, 0, h)
                pass_on(p, 0, 0, 1, h)
                pass_on(p, 0, 0, -1, h)
                to_mate(p, 0, h)
        for h in range(H):
            got(2, 0, h)
            pass_on(2, 0, 0, 1, h)
            pass_on(2, 0, 0, -1, h)
            pass_on(2, 0, 0, 2, h)
            to_mate(2, 0, h)
        for h in range(H):
            for q in (1, 3):
                got(0, q, h)
                to_mate(0, q, h)
        got_mate(0, 0)
        near = [(1, 0), (3, 0), (0, 3), (0, 1)]
        for p, q in near:
            got_mate(p, q)
        project_all([(0, 0)] + near)

        for d in range(1, 4):
            block = xz.at[l, ((z + d) % 4) * 2 + co]
            arrived(block, z_sem.at[l, d])
            send(block, block, zm_sem.at[l, d], mate)
        queries(z, xg[l, pl.ds(chip_of(0, 0) * 2, 2)])
        for h in range(H):
            for p in (1, 3):
                got(p, 1, h)
                pass_on(p, 1, 0, -1, h)
                to_mate(p, 1, h)
        for h in range(H):
            got(0, 2, h)
            to_mate(0, 2, h)
        for d in range(1, 4):
            pz = (z + d) % 4
            arrived(xz.at[l, pz * 2 + 1 - co], zm_sem.at[l, d])
            queries(pz, xz[l, pl.ds(pz * 2, 2)])
        middle = [(2, 0), (0, 2)]
        for p, q in middle:
            got_mate(p, q)
        project_all(middle)

        def attend(g, far):
            sums, marks = (so_far, sm_far) if far else (so, sm)
            row, count = (5, counts[1]) if far else (0, counts[0])

            def slot(s, top_before, mass_before):
                vals = vbuf[g, meta[row + 1, s]]
                scores = jnp.dot(
                    kbuf[g, meta[row + 1, s]], qbd[meta[row, s], g], preferred_element_type=f32
                )
                new = jnp.full((1, 256), meta[row + 2, s], jnp.int32) > 0
                if far:
                    start = meta[row + 3, s]
                    top_before = jnp.where(new, sm[start, 2 * g : 2 * g + 1, :], top_before)
                    mass_before = jnp.where(new, sm[start, 2 * g + 1 : 2 * g + 2, :], mass_before)
                else:
                    top_before = jnp.where(new, LOW, top_before)
                top = jnp.maximum(top_before, jnp.max(scores, axis=0, keepdims=True))
                keep = jnp.exp2((top_before - top) * SCALE)
                p = jnp.exp2((scores - top) * SCALE)
                mass = mass_before * keep + jnp.sum(p, axis=0, keepdims=True)
                marks[s + 1, 2 * g : 2 * g + 1, :] = top
                marks[s + 1, 2 * g + 1 : 2 * g + 2, :] = mass
                pb = p.astype(bf16)
                for hh in range(2):
                    at, half = slice(hh * HD, (hh + 1) * HD), slice(hh * 128, (hh + 1) * 128)
                    part = jnp.dot(vals[at, :], pb[:, half], preferred_element_type=f32)
                    before = sums[g, s, at, :]
                    if far:
                        before = jnp.where(new[:, :128], so[g, start, at, :], before)
                    sums[g, s + 1, at, :] = before * keep[:, half] + part
                return top, mass

            def steps(i, carry):
                for n in range(STEP[count]):
                    carry = slot(i * STEP[count] + n, *carry)
                return carry

            init = (jnp.full((1, 256), LOW, f32), jnp.zeros((1, 256), f32))
            lax.fori_loop(0, count // STEP[count], steps, init)

        def state(g, b):
            near, far = meta[4, b], meta[9, b]
            take = jnp.full((1, 128), far, jnp.int32) > 0
            sums = jnp.where(take, so_far[g, far], so[g, near])
            take = jnp.full((1, 256), far, jnp.int32) > 0
            marks = jnp.where(take, sm_far[far, 2 * g : 2 * g + 2, :], sm[near, 2 * g : 2 * g + 2, :])
            return sums.astype(bf16), marks

        for g in range(2):
            attend(g, False)

        for p, q in ((1, 3), (3, 3), (2, 1), (2, 3), (1, 2), (3, 2), (2, 2)):
            for h in range(H):
                got(p, q, h)
                to_mate(p, q, h)
        far = [(1, 1), (3, 1), (1, 3), (3, 3), (1, 2), (3, 2), (2, 1), (2, 3), (2, 2)]
        for p, q in far[:4]:
            got_mate(p, q)
        project_all(far[:4])
        for p, q in far[4:]:
            got_mate(p, q)
        project_all(far[4:])

        for g in range(2):
            attend(g, True)
            for n, (d, core) in enumerate([(d, core) for d in (2, 1, 3) for core in (0, 1)] + [(0, 1 - co)]):
                osend[l, g, n], msend[l, g, n] = state(g, ((z + d) % 4) * 2 + core)
                to, at = z_peer(d, core), z * 2 + co
                sem = ((-d) % 4) * 2 + co
                send(osend.at[l, g, n], orecv.at[l, g, at], o_sem.at[l, g, sem], to)
                send(msend.at[l, g, n], mrecv.at[l, g, at], m_sem.at[l, g, sem], to)
            orecv[l, g, z * 2 + co], mrecv[l, g, z * 2 + co] = state(g, z * 2 + co)

        for cp in weights[1:]:
            cp.wait()
        for g in range(2):
            for d, core in [(0, 1 - co)] + [(d, core) for d in (1, 3, 2) for core in (0, 1)]:
                at = ((z + d) % 4) * 2 + core
                arrived(orecv.at[l, g, at], o_sem.at[l, g, d * 2 + core])
                arrived(mrecv.at[l, g, at], m_sem.at[l, g, d * 2 + core])
            for core in range(2):
                tops = [mrecv[l, g, i * 2 + core, 0:1, :] for i in range(4)]
                top = jnp.maximum(jnp.maximum(tops[0], tops[1]), jnp.maximum(tops[2], tops[3]))
                shares = [jnp.exp2((tops[i] - top) * SCALE) for i in range(4)]
                mass = sum(shares[i] * mrecv[l, g, i * 2 + core, 1:2, :] for i in range(4))
                shares = [share / mass for share in shares]
                for hh in range(2):
                    at, half = slice(hh * HD, (hh + 1) * HD), slice(hh * 128, (hh + 1) * 128)
                    to = core * 256 + g * 128 + hh * HD
                    attn_t[to : to + HD, :] = sum(
                        orecv[l, g, i * 2 + core, at, :].astype(f32) * shares[i][:, half] for i in range(4)
                    ).astype(bf16)

        mixed = lax.dot_general(
            attn_t[...], wout[l], (((0,), (0,)), ((), ())), preferred_element_type=f32
        )
        hidden = normed(xg[l, own].astype(f32) + mixed, gain[l, 0:1, :], bias[l, 0:1, :]).astype(bf16)
        up = jax.nn.gelu(jnp.dot(hidden, wup[l], preferred_element_type=f32)).astype(bf16)
        down = jnp.dot(up, wdown[l], preferred_element_type=f32)
        result = normed(hidden.astype(f32) + down, gain[l, 1:2, :], bias[l, 1:2, :]).astype(bf16)

        @pl.when(l == 0)
        def _():
            xg[1, own] = result

        @pl.when(l == 1)
        def _():
            out_ref[...] = result

        assert len(sends) < NSEND
        for cp in sends:
            cp.wait_send()
        return carry

    lax.fori_loop(0, LAYERS, layer, 0)


def run_layers(counts, collective_id, meta, *arrays):
    vmem, bf16, f32 = pltpu.VMEM, jnp.bfloat16, jnp.float32
    dma = pltpu.SemaphoreType.DMA
    anywhere = pl.BlockSpec(memory_space=pl.ANY)
    whole = pl.BlockSpec(memory_space=pltpu.VMEM)
    near, far = counts[0] + 1, counts[1] + 1
    return pl.pallas_call(
        functools.partial(layers_kernel, counts),
        out_shape=jax.ShapeDtypeStruct((BLOCK, D), bf16),
        in_specs=[pl.BlockSpec(memory_space=pltpu.SMEM)] + [anywhere] * 5 + [whole] * 2,
        out_specs=whole,
        scratch_shapes=[
            vmem((2, 32, BLOCK, D), bf16),
            vmem((2, 8, BLOCK, D), bf16),
            vmem((2, 32, BLOCK, 128), bf16),
            vmem((2, 32, 128, BLOCK), bf16),
            vmem((8, 2, 128, 256), bf16),
            vmem((2, near, 128, 128), f32),
            vmem((near, 4, 256), f32),
            vmem((2, far, 128, 128), f32),
            vmem((far, 4, 256), f32),
            vmem((2, 2, 7, 128, 128), bf16),
            vmem((2, 2, 7, 2, 256), f32),
            vmem((2, 2, 8, 128, 128), bf16),
            vmem((2, 2, 8, 2, 256), f32),
            vmem((D, BLOCK), bf16),
            vmem((2, D, 3 * D), bf16),
            vmem((2, D, D), bf16),
            vmem((2, D, FF), bf16),
            vmem((2, FF, D), bf16),
            vmem((256, D), bf16),
            vmem((256, D), bf16),
            dma((1,)),
            dma((4, 2)),
            dma((2, 16 * H)),
            dma((2, 16 * H)),
            dma((2, 4)),
            dma((2, 4)),
            dma((2, 2, 8)),
            dma((2, 2, 8)),
            dma((2, NSEND)),
        ],
        compiler_params=pltpu.CompilerParams(
            collective_id=collective_id, has_side_effects=True, vmem_limit_bytes=(48 if counts == SHORT else 62) * 1024 * 1024
        ),
        name=f"layers_{near}",
    )(meta, *arrays)


def per_device(node_feats, block_mask, w_qkv, w_out, w_up, w_down, ln_gain, ln_bias):
    meta, fits = pl.pallas_call(
        lists_kernel,
        out_shape=(jax.ShapeDtypeStruct((16, SLOTS), jnp.int32), jax.ShapeDtypeStruct((1, 1), jnp.int32)),
        in_specs=[pl.BlockSpec(memory_space=pltpu.VMEM)],
        out_specs=(pl.BlockSpec(memory_space=pltpu.VMEM), pl.BlockSpec(memory_space=pltpu.SMEM)),
        name="lists",
    )(block_mask)
    return lax.cond(
        fits[0, 0] > 0,
        functools.partial(run_layers, SHORT, 0),
        functools.partial(run_layers, LONG, 1),
        meta, node_feats, w_qkv, w_out, w_up, w_down, ln_gain, ln_bias,
    )


def solution(mesh):
    placed = (P(("row", "col"), None), P(), P(), P(), P(), P(), P(), P())
    return jax.shard_map(
        per_device, mesh=mesh, in_specs=placed, out_specs=P(("row", "col"), None), check_vma=False
    )
```

```python
import functools
import math

import jax
import jax.numpy as jnp
from jax import lax
from jax.experimental import pallas as pl
from jax.experimental.pallas import tpu as pltpu
from jax.sharding import PartitionSpec as P

MESH = pl.DeviceIdType.MESH
D = 512
HEADS = 8
FF = 1024
BLOCK = 128
LAYERS = 2
HD = D // HEADS
LOW = -1e30
SCALE = math.log2(math.e) / math.sqrt(HD)
H = 1
NSEND = 104
SHORT = (36, 36)
LONG = (112, 144)
STEP = {36: 36, 112: 16, 144: 16}
SLOTS = 256


def in_line(a, b):
    same_x = (a >> 3) * 2 + (a & 1) == (b >> 3) * 2 + (b & 1)
    return jnp.where(same_x | (((a >> 1) & 3) == ((b >> 1) & 3)), 1.0, 0.0)


def lists_kernel(mask_ref, out_ref, fits_ref):
    r, c = lax.axis_index("row"), lax.axis_index("col")
    z, chip = r // 2, (r % 2) * 8 + c // 2
    f32 = jnp.float32
    mask = mask_ref[...].astype(f32)
    iota = lambda shape, d: lax.broadcasted_iota(jnp.int32, shape, d)
    one = lambda cond: jnp.where(cond, 1.0, 0.0).astype(f32)
    dims = lambda a, b: (((a,), (b,)), ((), ()))
    dot = lambda a, b, d: lax.dot_general(a, b, d, preferred_element_type=f32)
    plane_chip = one(((iota((16, 128), 1) & 31) >> 1) == iota((16, 128), 0))
    plane_z = one((iota((128, 8), 0) >> 5) == iota((128, 8), 1))
    close = in_line(iota((16, 128), 0), (iota((16, 128), 1) & 31) >> 1)
    linked = dot(plane_chip, mask, dims(1, 0))
    near_most = jnp.max(dot(linked * close, plane_z, dims(1, 0)))
    far_most = jnp.max(dot(linked * (1.0 - close), plane_z, dims(1, 0)))
    fits = (near_most <= SHORT[0]) & (far_most <= SHORT[1])
    fits_ref[0, 0] = fits.astype(jnp.int32)

    b = iota((8, 128), 0)
    query_sel = one(iota((8, 128), 1) == (b >> 1) * 32 + chip * 2 + (b & 1))
    key_sel = one(iota((128, 32), 0) == iota((128, 32), 1) + z * 32)
    sub = dot(key_sel, dot(mask, query_sel, dims(0, 1)), dims(0, 0))
    near = in_line(iota((32, 8), 0) >> 1, chip)
    earlier = one(iota((32, 32), 1) < iota((32, 32), 0))
    lanes = iota((32, SLOTS), 1).astype(f32)
    keys = iota((32, SLOTS), 0).astype(f32)
    lane = iota((1, SLOTS), 1).astype(f32)
    zero = jnp.zeros((1, SLOTS), f32)
    over_before = one(iota((8, 8), 0) < iota((8, 8), 1))
    spread = one(iota((8, SLOTS), 0) == iota((8, SLOTS), 1))
    rows, last = [], jnp.zeros((8, 8), f32)
    for group in (sub * near, sub * (1.0 - near)):
        q_row = k_row = n_row = p_row = zero
        totals = jnp.broadcast_to(jnp.sum(group, axis=0, keepdims=True), (8, 8))
        starts = dot(totals, over_before, dims(1, 0))
        ranks = dot(earlier, group, dims(1, 0)) + starts[0:1, :]
        for q in range(8):
            hit = jnp.where((ranks[:, q : q + 1] == lanes) & (group[:, q : q + 1] > 0.5), 1.0, 0.0)
            taken = jnp.sum(hit, axis=0, keepdims=True)
            q_row += taken * float(q)
            k_row += jnp.sum(hit * keys, axis=0, keepdims=True)
            fresh = jnp.where(lane == starts[0:1, q : q + 1], taken, 0.0)
            n_row += fresh
            p_row += fresh * last[0:1, q : q + 1]
        last = jnp.where(totals > 0.5, starts + totals, 0.0)
        rows += [q_row, k_row, n_row, p_row, dot(last, spread, dims(1, 0))[0:1, :]]
    for n, row in enumerate(rows):
        out_ref[n : n + 1, :] = row.astype(jnp.int32)
    out_ref[10:16, :] = jnp.zeros((6, SLOTS), jnp.int32)


def normed(values, gain, bias):
    center = values - jnp.mean(values, axis=-1, keepdims=True)
    spread = jnp.mean(center * center, axis=-1, keepdims=True)
    return center * lax.rsqrt(spread + 1e-05) * gain + bias


def layers_kernel(
    counts, meta, x_hbm, wqkv_hbm, wout_hbm, wup_hbm, wdown_hbm, gain, bias, out_ref,
    xg, xz, kbuf, vbuf, qbd, so, sm, so_far, sm_far, osend, msend, orecv, mrecv, attn_t,
    wqkv, wout, wup, wdown, wq_t, wv_t,
    in_sem, w_sem, own_sem, mate_sem, z_sem, zm_sem, o_sem, m_sem, send_sem,
):
    f32, bf16 = jnp.float32, jnp.bfloat16
    r, c = lax.axis_index("row"), lax.axis_index("col")
    z, y, co = r // 2, c // 4, c % 2
    x = (r % 2) * 2 + (c // 2) % 2
    rows_of = BLOCK // H

    def device(px, py, pz, pc):
        return (pz * 2 + px // 2, py * 4 + (px % 2) * 2 + pc)

    def place(p, q):
        dx, dy = p * (1 - co) + q * co, q * (1 - co) + p * co
        return (x + dx + 8) % 4, (y + dy + 8) % 4

    def chip_of(p, q):
        px, py = place(p, q)
        return (px // 2) * 8 + py * 2 + px % 2

    def block_of(p, q):
        return chip_of(p, q) * 2 + co

    def peer(p, q):
        px, py = place(p, q)
        return device(px, py, z, co)

    def z_peer(d, core):
        return device(x, y, (z + d) % 4, core)

    mate = device(x, y, z, 1 - co)
    own = block_of(0, 0)

    first = [
        pltpu.make_async_copy(x_hbm, xg.at[0, own], in_sem.at[0]),
    ]
    for cp in first:
        cp.start()

    def weight_copies(l):
        return [
            pltpu.make_async_copy(src.at[l], dst.at[l], w_sem.at[i, l])
            for i, (src, dst) in enumerate(
                ((wqkv_hbm, wqkv), (wout_hbm, wout), (wup_hbm, wup), (wdown_hbm, wdown))
            )
        ]

    for l in range(LAYERS):
        for cp in weight_copies(l):
            cp.start()

    barrier = pltpu.get_barrier_semaphore()
    others = [peer(1, 0), peer(-1, 0), peer(2, 0), peer(0, 1), peer(0, -1), peer(0, 2)]
    others += [z_peer(d, core) for d in (1, 2, 3) for core in (0, 1)] + [mate]
    for other in others:
        pl.semaphore_signal(barrier, inc=1, device_id=other, device_id_type=MESH)

    qbd[...] = jnp.zeros_like(qbd)
    for sums, marks in ((so, sm), (so_far, sm_far)):
        for g in range(2):
            sums[g, 0] = jnp.zeros((128, 128), f32)
            marks[0, 2 * g : 2 * g + 1, :] = jnp.full((1, 256), LOW, f32)
            marks[0, 2 * g + 1 : 2 * g + 2, :] = jnp.zeros((1, 256), f32)
    pl.semaphore_wait(barrier, len(others))
    for cp in first:
        cp.wait()

    def layer(l, carry):
        sends = []

        def send(src, dst, sem, to):
            cp = pltpu.make_async_remote_copy(
                src_ref=src, dst_ref=dst, send_sem=send_sem.at[l, len(sends)], recv_sem=sem,
                device_id=to, device_id_type=MESH,
            )
            cp.start()
            sends.append(cp)

        def index(p, q):
            return (p % 4) * 4 + q % 4

        def piece(block, h):
            return xg.at[l, block, pl.ds(h * rows_of, rows_of)]

        def pass_on(p, q, da, db, h):
            block = piece(block_of(p, q), h)
            send(block, block, own_sem.at[l, index(p - da, q - db) * H + h], peer(da, db))

        def to_mate(p, q, h):
            block = piece(block_of(p, q), h)
            send(block, block, mate_sem.at[l, index(p, q) * H + h], mate)

        def arrived(block, sem):
            pltpu.make_async_remote_copy(
                src_ref=block, dst_ref=block, send_sem=send_sem.at[l, NSEND - 1], recv_sem=sem,
                device_id=mate, device_id_type=MESH,
            ).wait_recv()

        def got(p, q, h):
            arrived(piece(block_of(p, q), h), own_sem.at[l, index(p, q) * H + h])

        def got_mate(p, q):
            for h in range(H):
                arrived(piece(chip_of(p, q) * 2 + 1 - co, h), mate_sem.at[l, index(q, p) * H + h])

        for h in range(H):
            pass_on(0, 0, 1, 0, h)
            pass_on(0, 0, -1, 0, h)
            pass_on(0, 0, 0, 1, h)
            pass_on(0, 0, 0, -1, h)
        for h in range(H):
            pass_on(0, 0, 2, 0, h)
            pass_on(0, 0, 0, 2, h)
        for h in range(H):
            to_mate(0, 0, h)
        for d in (1, 3, 2):
            send(xg.at[l, own], xz.at[l, z * 2 + co], z_sem.at[l, (-d) % 4], z_peer(d, co))

        weights = weight_copies(l)
        weights[0].wait()
        wq_t[...] = wqkv[l, :, pl.ds(pl.multiple_of(co * 256, 256), 256)].T
        wv_t[...] = wqkv[l, :, pl.ds(pl.multiple_of(2 * D + co * 256, 256), 256)].T

        def transposed_product(weight, rows):
            return lax.dot_general(weight, rows, (((1,), (1,)), ((), ())), preferred_element_type=f32).astype(bf16)

        def project(chip):
            rows = xg[l, pl.ds(chip * 2, 2)].reshape(2 * BLOCK, D)
            keys = jnp.dot(
                rows, wqkv[l, :, pl.ds(pl.multiple_of(D + co * 256, 256), 256)], preferred_element_type=f32
            ).astype(bf16)
            vals = transposed_product(wv_t[...], rows)
            for i in range(2):
                for g in range(2):
                    kbuf[g, chip * 2 + i] = keys[i * BLOCK : (i + 1) * BLOCK, g * 128 : (g + 1) * 128]
                    vbuf[g, chip * 2 + i] = vals[g * 128 : (g + 1) * 128, i * BLOCK : (i + 1) * BLOCK]

        def project_all(places):
            for p, q in places:
                project(chip_of(p, q))

        def queries(pz, rows):
            q_t = transposed_product(wq_t[...], rows.reshape(2 * BLOCK, D))
            for core in range(2):
                for h in range(4):
                    hh = h % 2
                    qbd[pz * 2 + core, h // 2, hh * HD : (hh + 1) * HD, hh * BLOCK : (hh + 1) * BLOCK] = q_t[
                        h * HD : (h + 1) * HD, core * BLOCK : (core + 1) * BLOCK
                    ]

        for h in range(H):
            for p in (1, 3):
                got(p, 0, h)
                pass_on(p, 0, 0, 1, h)
                pass_on(p, 0, 0, -1, h)
                to_mate(p, 0, h)
        for h in range(H):
            got(2, 0, h)
            pass_on(2, 0, 0, 1, h)
            pass_on(2, 0, 0, -1, h)
            pass_on(2, 0, 0, 2, h)
            to_mate(2, 0, h)
        for h in range(H):
            for q in (1, 3):
                got(0, q, h)
                to_mate(0, q, h)
        got_mate(0, 0)
        near = [(1, 0), (3, 0), (0, 3), (0, 1)]
        for p, q in near:
            got_mate(p, q)
        project_all([(0, 0)] + near)

        for d in range(1, 4):
            block = xz.at[l, ((z + d) % 4) * 2 + co]
            arrived(block, z_sem.at[l, d])
            send(block, block, zm_sem.at[l, d], mate)
        queries(z, xg[l, pl.ds(chip_of(0, 0) * 2, 2)])
        for h in range(H):
            for p in (1, 3):
                got(p, 1, h)
                pass_on(p, 1, 0, -1, h)
                to_mate(p, 1, h)
        for h in range(H):
            got(0, 2, h)
            to_mate(0, 2, h)
        for d in range(1, 4):
            pz = (z + d) % 4
            arrived(xz.at[l, pz * 2 + 1 - co], zm_sem.at[l, d])
            queries(pz, xz[l, pl.ds(pz * 2, 2)])
        middle = [(2, 0), (0, 2)]
        for p, q in middle:
            got_mate(p, q)
        project_all(middle)

        def attend(g, far):
            sums, marks = (so_far, sm_far) if far else (so, sm)
            row, count = (5, counts[1]) if far else (0, counts[0])

            def slot(s, top_before, mass_before):
                vals = vbuf[g, meta[row + 1, s]]
                scores = jnp.dot(
                    kbuf[g, meta[row + 1, s]], qbd[meta[row, s], g], preferred_element_type=f32
                )
                new = jnp.full((1, 256), meta[row + 2, s], jnp.int32) > 0
                if far:
                    start = meta[row + 3, s]
                    top_before = jnp.where(new, sm[start, 2 * g : 2 * g + 1, :], top_before)
                    mass_before = jnp.where(new, sm[start, 2 * g + 1 : 2 * g + 2, :], mass_before)
                else:
                    top_before = jnp.where(new, LOW, top_before)
                top = jnp.maximum(top_before, jnp.max(scores, axis=0, keepdims=True))
                keep = jnp.exp2((top_before - top) * SCALE)
                p = jnp.exp2((scores - top) * SCALE)
                mass = mass_before * keep + jnp.sum(p, axis=0, keepdims=True)
                marks[s + 1, 2 * g : 2 * g + 1, :] = top
                marks[s + 1, 2 * g + 1 : 2 * g + 2, :] = mass
                pb = p.astype(bf16)
                for hh in range(2):
                    at, half = slice(hh * HD, (hh + 1) * HD), slice(hh * 128, (hh + 1) * 128)
                    part = jnp.dot(vals[at, :], pb[:, half], preferred_element_type=f32)
                    before = sums[g, s, at, :]
                    if far:
                        before = jnp.where(new[:, :128], so[g, start, at, :], before)
                    sums[g, s + 1, at, :] = before * keep[:, half] + part
                return top, mass

            def steps(i, carry):
                for n in range(STEP[count]):
                    carry = slot(i * STEP[count] + n, *carry)
                return carry

            init = (jnp.full((1, 256), LOW, f32), jnp.zeros((1, 256), f32))
            lax.fori_loop(0, count // STEP[count], steps, init)

        def state(g, b):
            near, far = meta[4, b], meta[9, b]
            take = jnp.full((1, 128), far, jnp.int32) > 0
            sums = jnp.where(take, so_far[g, far], so[g, near])
            take = jnp.full((1, 256), far, jnp.int32) > 0
            marks = jnp.where(take, sm_far[far, 2 * g : 2 * g + 2, :], sm[near, 2 * g : 2 * g + 2, :])
            return sums.astype(bf16), marks

        for g in range(2):
            attend(g, False)

        for p, q in ((1, 3), (3, 3), (2, 1), (2, 3)):
            for h in range(H):
                got(p, q, h)
                to_mate(p, q, h)
        far = [(1, 1), (3, 1), (1, 3), (3, 3), (1, 2), (3, 2), (2, 1), (2, 3), (2, 2)]
        for p, q in far[:4]:
            got_mate(p, q)
        project_all(far[:4])
        for p, q in ((1, 2), (3, 2), (2, 2)):
            for h in range(H):
                got(p, q, h)
                to_mate(p, q, h)
        for p, q in far[4:]:
            got_mate(p, q)
        project_all(far[4:])

        for g in range(2):
            attend(g, True)
            for n, (d, core) in enumerate([(d, core) for d in (2, 1, 3) for core in (0, 1)] + [(0, 1 - co)]):
                osend[l, g, n], msend[l, g, n] = state(g, ((z + d) % 4) * 2 + core)
                to, at = z_peer(d, core), z * 2 + co
                sem = ((-d) % 4) * 2 + co
                send(osend.at[l, g, n], orecv.at[l, g, at], o_sem.at[l, g, sem], to)
                send(msend.at[l, g, n], mrecv.at[l, g, at], m_sem.at[l, g, sem], to)
            orecv[l, g, z * 2 + co], mrecv[l, g, z * 2 + co] = state(g, z * 2 + co)

        for cp in weights[1:]:
            cp.wait()
        for g in range(2):
            for d, core in [(0, 1 - co)] + [(d, core) for d in (1, 3, 2) for core in (0, 1)]:
                at = ((z + d) % 4) * 2 + core
                arrived(orecv.at[l, g, at], o_sem.at[l, g, d * 2 + core])
                arrived(mrecv.at[l, g, at], m_sem.at[l, g, d * 2 + core])
            for core in range(2):
                tops = [mrecv[l, g, i * 2 + core, 0:1, :] for i in range(4)]
                top = jnp.maximum(jnp.maximum(tops[0], tops[1]), jnp.maximum(tops[2], tops[3]))
                shares = [jnp.exp2((tops[i] - top) * SCALE) for i in range(4)]
                mass = sum(shares[i] * mrecv[l, g, i * 2 + core, 1:2, :] for i in range(4))
                shares = [share / mass for share in shares]
                for hh in range(2):
                    at, half = slice(hh * HD, (hh + 1) * HD), slice(hh * 128, (hh + 1) * 128)
                    to = core * 256 + g * 128 + hh * HD
                    attn_t[to : to + HD, :] = sum(
                        orecv[l, g, i * 2 + core, at, :].astype(f32) * shares[i][:, half] for i in range(4)
                    ).astype(bf16)

        mixed = lax.dot_general(
            attn_t[...], wout[l], (((0,), (0,)), ((), ())), preferred_element_type=f32
        )
        hidden = normed(xg[l, own].astype(f32) + mixed, gain[l, 0:1, :], bias[l, 0:1, :]).astype(bf16)
        up = jax.nn.gelu(jnp.dot(hidden, wup[l], preferred_element_type=f32)).astype(bf16)
        down = jnp.dot(up, wdown[l], preferred_element_type=f32)
        result = normed(hidden.astype(f32) + down, gain[l, 1:2, :], bias[l, 1:2, :]).astype(bf16)

        @pl.when(l == 0)
        def _():
            xg[1, own] = result

        @pl.when(l == 1)
        def _():
            out_ref[...] = result

        assert len(sends) < NSEND
        for cp in sends:
            cp.wait_send()
        return carry

    lax.fori_loop(0, LAYERS, layer, 0)


def run_layers(counts, collective_id, meta, *arrays):
    vmem, bf16, f32 = pltpu.VMEM, jnp.bfloat16, jnp.float32
    dma = pltpu.SemaphoreType.DMA
    anywhere = pl.BlockSpec(memory_space=pl.ANY)
    whole = pl.BlockSpec(memory_space=pltpu.VMEM)
    near, far = counts[0] + 1, counts[1] + 1
    return pl.pallas_call(
        functools.partial(layers_kernel, counts),
        out_shape=jax.ShapeDtypeStruct((BLOCK, D), bf16),
        in_specs=[pl.BlockSpec(memory_space=pltpu.SMEM)] + [anywhere] * 5 + [whole] * 2,
        out_specs=whole,
        scratch_shapes=[
            vmem((2, 32, BLOCK, D), bf16),
            vmem((2, 8, BLOCK, D), bf16),
            vmem((2, 32, BLOCK, 128), bf16),
            vmem((2, 32, 128, BLOCK), bf16),
            vmem((8, 2, 128, 256), bf16),
            vmem((2, near, 128, 128), f32),
            vmem((near, 4, 256), f32),
            vmem((2, far, 128, 128), f32),
            vmem((far, 4, 256), f32),
            vmem((2, 2, 7, 128, 128), bf16),
            vmem((2, 2, 7, 2, 256), f32),
            vmem((2, 2, 8, 128, 128), bf16),
            vmem((2, 2, 8, 2, 256), f32),
            vmem((D, BLOCK), bf16),
            vmem((2, D, 3 * D), bf16),
            vmem((2, D, D), bf16),
            vmem((2, D, FF), bf16),
            vmem((2, FF, D), bf16),
            vmem((256, D), bf16),
            vmem((256, D), bf16),
            dma((1,)),
            dma((4, 2)),
            dma((2, 16 * H)),
            dma((2, 16 * H)),
            dma((2, 4)),
            dma((2, 4)),
            dma((2, 2, 8)),
            dma((2, 2, 8)),
            dma((2, NSEND)),
        ],
        compiler_params=pltpu.CompilerParams(
            collective_id=collective_id, has_side_effects=True, vmem_limit_bytes=(48 if counts == SHORT else 62) * 1024 * 1024
        ),
        name=f"layers_{near}",
    )(meta, *arrays)


def per_device(node_feats, block_mask, w_qkv, w_out, w_up, w_down, ln_gain, ln_bias):
    meta, fits = pl.pallas_call(
        lists_kernel,
        out_shape=(jax.ShapeDtypeStruct((16, SLOTS), jnp.int32), jax.ShapeDtypeStruct((1, 1), jnp.int32)),
        in_specs=[pl.BlockSpec(memory_space=pltpu.VMEM)],
        out_specs=(pl.BlockSpec(memory_space=pltpu.VMEM), pl.BlockSpec(memory_space=pltpu.SMEM)),
        name="lists",
    )(block_mask)
    return lax.cond(
        fits[0, 0] > 0,
        functools.partial(run_layers, SHORT, 0),
        functools.partial(run_layers, LONG, 1),
        meta, node_feats, w_qkv, w_out, w_up, w_down, ln_gain, ln_bias,
    )


def solution(mesh):
    placed = (P(("row", "col"), None), P(), P(), P(), P(), P(), P(), P())
    return jax.shard_map(
        per_device, mesh=mesh, in_specs=placed, out_specs=P(("row", "col"), None), check_vma=False
    )
```
